256 devices in a mesh: blk: 64 (over z, y, x_hi), grp: 4 (over x_lo, core).
Axes of the slice: x: 4 (x_hi: 2, x_lo: 2; x = x_hi * 2 + x_lo), y: 4, z: 8, core: 2. Of those that a mesh axis runs over, the one named last changes fastest.
Arguments:
- start_state: float32 [512, 4096], P(('blk', 'grp')), may hold values from -6 to 6
- start_log_weight: float32 [512], P(('blk', 'grp')), may hold values from -10 to 330
- noise: bfloat16 [3, 512, 4096], P(None, ('blk', 'grp')), may hold values from -6 to 6
- first_weight: bfloat16 [14336, 4096], P('blk'), may hold values from -0.09375 to 0.09375
- second_weight: bfloat16 [14336, 4096], P('blk'), may hold values from -0.09375 to 0.09375
- third_weight: bfloat16 [14336, 4096], P('blk'), may hold values from -0.09375 to 0.09375
Outputs:
- final_state: float32 [512, 4096], P(('blk', 'grp'))
- log_weight: float32 [512], P(('blk', 'grp'))
- log_ratio: float32 [], replicated
The draws below stay inside these ranges and needn't reach their ends.
All inputs are finite; a program needn't handle non-finite values.
Results may differ from the reference program's by a relative error of at most 0.00074.
Values may be sent and summed in bfloat16 or wider, within the bound.
A program may use at most 64 MiB of HBM per device.

```python
import math
import jax
import jax.numpy as jnp
from jax import lax

D = 4096
FF = 14336
STEPS = 3
CHAINS = 512


def draw_start_log_weight(key, part):
    base_key = jax.random.fold_in(key, 11)
    level_key = jax.random.fold_in(key, 12)
    order_key = jax.random.fold_in(key, 13)
    spread_key = jax.random.fold_in(key, 14)
    values = 2.0 * jax.random.normal(base_key, (CHAINS,), jnp.float32)
    values = jnp.clip(values, -8.0, 8.0)
    level = jax.random.uniform(level_key, (), jnp.float32, 105.0, 140.0)
    chosen = jax.random.permutation(order_key, CHAINS)[:3]
    offsets = jnp.array([0.0, 1.5, 2.7], jnp.float32) + jax.random.uniform(spread_key, (3,), jnp.float32, 0.0, 0.2)
    values = values.at[chosen].set(level - offsets)
    return values.astype(jnp.float32)


def block_levels(rng, extent, pieces, least, largest):
    def one(dim, shards_of):
        draws = jax.random.uniform(jax.random.fold_in(jax.random.fold_in(rng, 6), dim), (shards_of,), jnp.float32, least / len(pieces), largest / len(pieces))
        return jnp.repeat(jnp.exp(draws), extent[dim] // shards_of).reshape((-1,) + (1,) * (len(extent) - dim - 1))

    gain = one(*pieces[0])
    for cut in pieces[1:]:
        gain = gain * one(*cut)
    return gain


def bell_draw(stream_key, shape, scale, limit, pieces=(), dtype=jnp.bfloat16):
    gain = block_levels(stream_key, shape, pieces, -0.22, 0.18) if pieces else 1.0
    values = jax.random.normal(stream_key, shape, jnp.float32) * scale * gain
    return jnp.minimum(jnp.maximum(values, -limit), limit).astype(dtype)


def setup_inputs(seed: int = 0) -> dict:
    arg_keys = jax.random.split(jax.random.key(seed), 7)
    return {
        "start_state": bell_draw(arg_keys[0], (CHAINS, D), 1.0, 6.0, ((0, 256),), jnp.float32),
        "start_log_weight": draw_start_log_weight(jax.random.fold_in(arg_keys[6], 71), 0),
        "noise": bell_draw(arg_keys[2], (STEPS, CHAINS, D), 1.0, 6.0, ((1, 256),)),
        "first_weight": bell_draw(arg_keys[3], (FF, D), D ** -0.5, 0.09375, ((0, 64),)),
        "second_weight": bell_draw(arg_keys[4], (FF, D), D ** -0.5, 0.09375, ((0, 64),)),
        "third_weight": bell_draw(arg_keys[5], (FF, D), D ** -0.5, 0.09375, ((0, 64),)),
    }


def reference(start_state, start_log_weight, noise, first_weight, second_weight, third_weight):
    state = start_state
    log_weight = start_log_weight
    dims = (((1,), (1,)), ((), ()))
    for step in range(STEPS):
        rounded = state.astype(jnp.bfloat16)
        pre_a = lax.dot_general(rounded, first_weight, dims, preferred_element_type=jnp.float32)
        pre_b = lax.dot_general(rounded, second_weight, dims, preferred_element_type=jnp.float32)
        pre_c = lax.dot_general(rounded, third_weight, dims, preferred_element_type=jnp.float32)
        soft = jax.nn.softplus(pre_a)
        tan_b = jnp.tanh(pre_b)
        energy = lax.optimization_barrier(jnp.sum(soft * tan_b * pre_c, axis=1))
        factor_a = (jax.nn.sigmoid(pre_a) * tan_b * pre_c).astype(jnp.bfloat16)
        factor_b = (soft * (1.0 - tan_b * tan_b) * pre_c).astype(jnp.bfloat16)
        factor_c = (soft * tan_b).astype(jnp.bfloat16)
        gradient = jnp.dot(factor_a, first_weight, preferred_element_type=jnp.float32)
        gradient = gradient + jnp.dot(factor_b, second_weight, preferred_element_type=jnp.float32)
        gradient = gradient + jnp.dot(factor_c, third_weight, preferred_element_type=jnp.float32)
        log_weight = log_weight - energy / STEPS
        beta = (step + 1) / STEPS
        state = state - 0.05 * (state + beta * gradient) + math.sqrt(0.1) * noise[step].astype(jnp.float32)
    top = jnp.max(log_weight)
    total = jnp.sum(jnp.exp(log_weight - top))
    log_ratio = top + jnp.log(total) - math.log(CHAINS)
    return (state, log_weight, log_ratio)
```

```python
import math

import jax
import jax.numpy as jnp
from jax import lax
from jax.experimental import pallas as pl
from jax.experimental.pallas import tpu as pltpu
from jax.sharding import Mesh
from jax.sharding import PartitionSpec as P

BLK = ("blk_0", "blk_1", "blk_2")
BLK_GRP = ("blk_0", "blk_1", "blk_2", "grp_0", "grp_1")
AXES = BLK_GRP
MESH = pl.DeviceIdType.MESH
F32 = jnp.float32
BF16 = jnp.bfloat16

NZ, NY, NX = 8, 4, 2
PEERS = NY * NX
OWN = 2
BLOCK = OWN * NZ
ROWS = PEERS * BLOCK
STEPS = 3
D = 4096
CHUNK = D // NZ
TILES = CHUNK // 128
PAD = 256
LAG_OWN, LAG_PASS, LAG_USE = 2, 4, 6


def rem(a, n):
    return lax.rem(a, n)


def kernel(
    start_ref, slw_ref, noise_ref, w1_ref, w2_ref, w3_ref,
    out_ref, lw_ref, lr_ref,
    w, s_all, g_all, rx, zs, zx, zown, state, acc, fac, ener, esum,
    ipack, iall, npack, nall, fsend, fall, e1, ex, e2, ez, e3, el,
    wsem, agx, agz, rxs, zxs, one, snd, sndg,
):
    z, y, xh, xl, core = (lax.axis_index(name) for name in AXES)
    b = y * NX + xh
    width = w1_ref.shape[0]
    mine = pl.ds(pl.multiple_of(b * BLOCK, BLOCK), BLOCK)

    def zpeer(dz):
        return (rem(z + dz, NZ), y, xh, xl, core)

    def xypeer(rel):
        dy, dx = divmod(rel, NX)
        return (z, rem(y + dy, NY), rem(xh + dx, NX), rem(xl + dx, NX), core)

    def gpeer(k):
        dl, dc = divmod(k, 2)
        return (z, y, xh, rem(xl + dl, 2), rem(core + dc, 2))

    def push(src, dst, send, recv, to):
        pltpu.make_async_remote_copy(
            src_ref=src, dst_ref=dst, send_sem=send, recv_sem=recv, device_id=to, device_id_type=MESH
        ).start()

    def arrived(ref, recv):
        pltpu.make_async_remote_copy(
            src_ref=ref, dst_ref=ref, send_sem=snd.at[0], recv_sem=recv,
            device_id=zpeer(1), device_id_type=MESH,
        ).wait_recv()

    def left(ref, send):
        pltpu.make_async_remote_copy(
            src_ref=ref, dst_ref=ref, send_sem=send, recv_sem=one.at[0],
            device_id=zpeer(1), device_id_type=MESH,
        ).wait_send()

    weights = (w1_ref, w2_ref, w3_ref)

    def weight_copy(j, k):
        cols = pl.ds(pl.multiple_of(j * CHUNK, CHUNK), CHUNK)
        return pltpu.make_async_copy(
            weights[k].at[:, cols], w.at[j, k, pl.ds(0, width), :], wsem.at[j, k]
        )

    barrier = pltpu.get_barrier_semaphore()
    greeted = [zpeer(d) for d in range(1, NZ)] + [xypeer(r) for r in range(1, PEERS)] + [gpeer(k) for k in range(1, 4)]
    for to in greeted:
        pl.semaphore_signal(barrier, inc=1, device_id=to, device_id_type=MESH)

    @pl.loop(0, NZ)
    def _(j):
        for k in range(3):
            weight_copy(j, k).start()

    for t in range(D // 128):
        v = start_ref[:, t * 128 : (t + 1) * 128]
        ipack[t : t + 1, :] = v[0:1]
        ipack[32 + t : 33 + t, :] = v[1:2]
    iall[pl.ds(pl.multiple_of(z * 64, 64), 64), :] = ipack[...]

    pl.semaphore_wait(barrier, len(greeted))

    for dz in range(1, NZ):
        push(ipack, iall.at[pl.ds(pl.multiple_of(z * 64, 64), 64), :], snd.at[0], one.at[0], zpeer(dz))

    for k in range(STEPS):
        for t in range(D // 128):
            v = noise_ref[k, :, t * 128 : (t + 1) * 128].astype(F32)
            r = (k * TILES + t % TILES) * 2
            npack[t // TILES, r : r + 2, :] = v
    nall[pl.ds(pl.multiple_of(z * 24, 8), 24), :] = npack[z]
    for dz in range(1, NZ):
        to = rem(z + dz, NZ)
        push(npack.at[to], nall.at[pl.ds(pl.multiple_of(z * 24, 8), 24), :], snd.at[1], one.at[1], zpeer(dz))

    @pl.loop(0, NZ)
    def _(j):
        for k in range(3):
            w[j, k, width:PAD, :] = jnp.zeros((PAD - width, CHUNK), BF16)

    esum[...] = jnp.zeros_like(esum)

    def spread(n, j):
        for rel in range(1, PEERS):
            push(s_all.at[n, j, mine, :], s_all.at[n, j, mine, :], snd.at[2], agx.at[n, j], xypeer(rel))

    def forward(n, j):
        arrived(s_all.at[n, j, pl.ds(0, ROWS - BLOCK), :], agx.at[n, j])
        rows = s_all[n, j]
        for k in range(3):
            term = lax.dot_general(rows, w[j, k], (((1,), (1,)), ((), ())), preferred_element_type=F32)

            @pl.when(j == 0)
            def _():
                acc[k] = term

            @pl.when(j != 0)
            def _():
                acc[k] += term

    def start_tile(t):
        lo = iall[pl.ds(t, NZ, stride=64), :]
        hi = iall[pl.ds(32 + t, NZ, stride=64), :]
        return jnp.concatenate([lo, hi], axis=0)

    arrived(iall.at[pl.ds(0, 64 * (NZ - 1)), :], one.at[0])

    @pl.loop(0, NZ)
    def _(j):
        for tt in range(TILES):
            s_all[0, j, mine, tt * 128 : (tt + 1) * 128] = start_tile(j * TILES + tt).astype(BF16)
        spread(0, j)

    for tt in range(TILES):
        state[:, tt * 128 : (tt + 1) * 128] = start_tile(z * TILES + tt)

    @pl.loop(0, NZ)
    def _(j):
        for k in range(3):
            weight_copy(j, k).wait()
        forward(0, j)

    arrived(nall.at[pl.ds(0, 24 * (NZ - 1)), :], one.at[1])

    lane = lax.broadcasted_iota(jnp.int32, (1, ROWS), 1)

    def energy_out():
        v = esum[...] / STEPS
        for i in range(OWN):
            v = v - jnp.where(lane == b * BLOCK + i * NZ + z, slw_ref[i], 0.0)
        e1[...] = jnp.broadcast_to(v, e1.shape)
        for rel in range(1, PEERS):
            push(e1, ex.at[rel - 1], snd.at[5], one.at[3], xypeer(rel))

    def energy_mid():
        arrived(ex, one.at[3])
        total = e1[...]
        for k in range(PEERS - 1):
            total = total + ex[k]
        e2[...] = total
        for dz in range(1, NZ):
            push(e2, ez.at[dz - 1], snd.at[6], one.at[4], zpeer(dz))

    def energy_end():
        arrived(ez, one.at[4])
        total = e2[...]
        for k in range(NZ - 1):
            total = total + ez[k]
        e3[...] = -total
        for k in range(1, 4):
            push(e3, el.at[k - 1], snd.at[7], one.at[5], gpeer(k))

    def step(n, carry):
        last = n == STEPS - 1

        @pl.loop(0, 4)
        def _(q):
            r = pl.ds(pl.multiple_of(q * 32, 32), 32)
            pa, pb, pc = acc[0, r], acc[1, r], acc[2, r]
            e = jnp.exp(-jnp.abs(pa))
            soft = jnp.maximum(pa, 0.0) + jnp.log1p(e)
            inv = 1.0 / (1.0 + e)
            sig = jnp.where(pa >= 0, inv, e * inv)
            tan = jnp.tanh(pb)
            fac[r, 0:PAD] = (sig * tan * pc).astype(BF16)
            fac[r, PAD : 2 * PAD] = (soft * (1.0 - tan * tan) * pc).astype(BF16)
            st = soft * tan
            fac[r, 2 * PAD :] = st.astype(BF16)
            en = st * pc
            ener[r, :] = en[:, :128] + en[:, 128:]

        @pl.loop(0, NZ)
        def _(j):
            g = jnp.dot(fac[...], w[j].reshape(3 * PAD, CHUNK), preferred_element_type=F32)
            g_all[n, j] = g.astype(BF16)
            for rel in range(1, PEERS):
                dy, dx = divmod(rel, NX)
                to = rem(y + dy, NY) * NX + rem(xh + dx, NX)
                rows = pl.ds(pl.multiple_of(to * BLOCK, BLOCK), BLOCK)
                push(g_all.at[n, j, rows, :], rx.at[n, j, rel - 1], sndg.at[n], rxs.at[n, j], xypeer(rel))

        esum[...] += jnp.sum(ener[...].T, axis=0, keepdims=True)

        @pl.when(last)
        def _():
            energy_out()
            energy_mid()

        def mix(it, carry):
            @pl.when(it < NZ)
            def _():
                arrived(rx.at[n, it], rxs.at[n, it])
                total = g_all[n, it, mine, :].astype(F32)
                for k in range(PEERS - 1):
                    total = total + rx[n, it, k].astype(F32)

                @pl.when(it == z)
                def _():
                    zown[...] = total

                @pl.when(it != z)
                def _():
                    zs[n, it] = total.astype(BF16)
                    dz = rem(it - z + NZ, NZ)
                    push(zs.at[n, it], zx.at[n, dz - 1], snd.at[3], zxs.at[n], (it, y, xh, xl, core))

            @pl.when(it - LAG_OWN == z)
            def _():
                arrived(zx.at[n], zxs.at[n])
                grad = zown[...]
                for k in range(NZ - 1):
                    grad = grad + zx[n, k].astype(F32)
                beta = (n + 1).astype(F32) / STEPS
                news = []
                for tt in range(TILES):
                    cols = slice(tt * 128, (tt + 1) * 128)
                    row = (n * TILES + tt) * 2
                    extra = jnp.concatenate(
                        [nall[pl.ds(row, NZ, stride=24), :], nall[pl.ds(row + 1, NZ, stride=24), :]], axis=0
                    )
                    old = state[:, cols]
                    new = old - 0.05 * (old + beta * grad[:, cols]) + math.sqrt(0.1) * extra
                    state[:, cols] = new

                @pl.when(jnp.logical_not(last))
                def _():
                    s_all[n + 1, z, mine, :] = state[...].astype(BF16)
                    for dz in range(1, NZ):
                        push(s_all.at[n + 1, z, mine, :], s_all.at[n + 1, z, mine, :], snd.at[4], agz.at[n, z], zpeer(dz))
                    spread(n + 1, z)

            @pl.when(jnp.logical_not(last))
            def _():
                jp = it - LAG_PASS

                @pl.when((jp >= 0) & (jp < NZ) & (jp != z))
                def _():
                    arrived(s_all.at[n + 1, jp, mine, :], agz.at[n, jp])
                    spread(n + 1, jp)

                ju = it - LAG_USE

                @pl.when((ju >= 0) & (ju < NZ))
                def _():
                    forward(n + 1, ju)

            return carry

        lax.fori_loop(0, jnp.where(last, NZ + LAG_OWN, NZ + LAG_USE), mix, 0)
        return carry

    lax.fori_loop(0, STEPS, step, 0)

    for i in range(OWN):
        for tt in range(TILES):
            fsend[pl.ds(i * TILES + tt, NZ, stride=8), :] = state[i * NZ : (i + 1) * NZ, tt * 128 : (tt + 1) * 128]
    for dz in range(1, NZ):
        to = rem(z + dz, NZ)
        push(fsend.at[pl.ds(pl.multiple_of(to * 8, 8), 8), :], fall.at[z], snd.at[8], one.at[2], zpeer(dz))
    fall[z] = fsend[pl.ds(pl.multiple_of(z * 8, 8), 8), :]
    energy_end()
    arrived(el, one.at[5])
    lws = [e3[0:1]] + [el[k, 0:1] for k in range(3)]
    top = jnp.max(jnp.maximum(jnp.maximum(lws[0], lws[1]), jnp.maximum(lws[2], lws[3])))
    total = jnp.sum(sum(jnp.exp(v - top) for v in lws), axis=1, keepdims=True)
    chains = ROWS * 4
    lr_ref[0] = jnp.max(top + jnp.log(total) - math.log(chains))
    for i in range(OWN):
        lw_ref[i] = jnp.sum(jnp.where(lane == b * BLOCK + i * NZ + z, lws[0], 0.0))
    arrived(fall.at[pl.ds(0, NZ - 1)], one.at[2])
    for zz in range(NZ):
        for i in range(OWN):
            for tt in range(TILES):
                c = (zz * TILES + tt) * 128
                out_ref[i : i + 1, c : c + 128] = fall[zz, i * TILES + tt : i * TILES + tt + 1, :]

    left(iall.at[pl.ds(0, 64 * (NZ - 1)), :], snd.at[0])
    left(npack.at[pl.ds(0, NZ - 1)], snd.at[1])
    left(s_all.at[:, :, pl.ds(0, ROWS - BLOCK), :], snd.at[2])
    left(zs.at[:, pl.ds(0, NZ - 1)], snd.at[3])
    left(zx.at[pl.ds(0, STEPS - 1)], snd.at[4])
    left(ex, snd.at[5])
    left(ez, snd.at[6])
    left(el, snd.at[7])
    left(fall.at[pl.ds(0, NZ - 1)], snd.at[8])
    for n in range(STEPS):
        left(g_all.at[n, :, pl.ds(0, ROWS - BLOCK), :], sndg.at[n])


def per_device(start_state, start_log_weight, noise, first_weight, second_weight, third_weight):
    vmem = pl.BlockSpec(memory_space=pltpu.VMEM)
    smem = pl.BlockSpec(memory_space=pltpu.SMEM)
    hbm = pl.BlockSpec(memory_space=pl.ANY)
    tile = (8, 128)
    state, log_weight, log_ratio = pl.pallas_call(
        kernel,
        out_shape=(
            jax.ShapeDtypeStruct((OWN, D), F32),
            jax.ShapeDtypeStruct((OWN,), F32),
            jax.ShapeDtypeStruct((1,), F32),
        ),
        in_specs=[vmem, smem, vmem, hbm, hbm, hbm],
        out_specs=(vmem, smem, smem),
        scratch_shapes=[
            pltpu.VMEM((NZ, 3, PAD, CHUNK), BF16),
            pltpu.VMEM((STEPS, NZ, ROWS, CHUNK), BF16),
            pltpu.VMEM((STEPS, NZ, ROWS, CHUNK), BF16),
            pltpu.VMEM((STEPS, NZ, PEERS - 1, BLOCK, CHUNK), BF16),
            pltpu.VMEM((STEPS, NZ, BLOCK, CHUNK), BF16),
            pltpu.VMEM((STEPS, NZ - 1, BLOCK, CHUNK), BF16),
            pltpu.VMEM((BLOCK, CHUNK), F32),
            pltpu.VMEM((BLOCK, CHUNK), F32),
            pltpu.VMEM((3, ROWS, PAD), F32),
            pltpu.VMEM((ROWS, 3 * PAD), BF16),
            pltpu.VMEM((ROWS, 128), F32),
            pltpu.VMEM((1, ROWS), F32),
            pltpu.VMEM((64, 128), F32),
            pltpu.VMEM((64 * NZ, 128), F32),
            pltpu.VMEM((NZ, 24, 128), F32),
            pltpu.VMEM((24 * NZ, 128), F32),
            pltpu.VMEM((64, 128), F32),
            pltpu.VMEM((NZ, 8, 128), F32),
            pltpu.VMEM(tile, F32),
            pltpu.VMEM((PEERS - 1, *tile), F32),
            pltpu.VMEM(tile, F32),
            pltpu.VMEM((NZ - 1, *tile), F32),
            pltpu.VMEM(tile, F32),
            pltpu.VMEM((3, *tile), F32),
            pltpu.SemaphoreType.DMA((NZ, 3)),
            pltpu.SemaphoreType.DMA((STEPS, NZ)),
            pltpu.SemaphoreType.DMA((STEPS - 1, NZ)),
            pltpu.SemaphoreType.DMA((STEPS, NZ)),
            pltpu.SemaphoreType.DMA((STEPS,)),
            pltpu.SemaphoreType.DMA((6,)),
            pltpu.SemaphoreType.DMA((9,)),
            pltpu.SemaphoreType.DMA((STEPS,)),
        ],
        compiler_params=pltpu.CompilerParams(
            collective_id=0, has_side_effects=True, vmem_limit_bytes=48 << 20
        ),
    )(start_state, start_log_weight, noise, first_weight, second_weight, third_weight)
    return state, log_weight, log_ratio[0]


def solution(mesh):
    torus = Mesh(mesh.devices.reshape(8, 4, 2, 2, 2), AXES)
    placed = (
        P(BLK_GRP, None),
        P(BLK_GRP),
        P(None, BLK_GRP, None),
        P(BLK, None),
        P(BLK, None),
        P(BLK, None),
    )
    return jax.shard_map(
        per_device,
        mesh=torus,
        in_specs=placed,
        out_specs=(P(BLK_GRP, None), P(BLK_GRP), P()),
        check_vma=False,
    )
```

```python
import math

import jax
import jax.numpy as jnp
from jax import lax
from jax.experimental import pallas as pl
from jax.experimental.pallas import tpu as pltpu
from jax.sharding import Mesh
from jax.sharding import PartitionSpec as P

BLK = ("blk_0", "blk_1", "blk_2")
BLK_GRP = ("blk_0", "blk_1", "blk_2", "grp_0", "grp_1")
AXES = BLK_GRP
MESH = pl.DeviceIdType.MESH
F32 = jnp.float32
BF16 = jnp.bfloat16

NZ, NY, NX = 8, 4, 2
OWN = 2
BLOCK = NX * NZ
ROWS = NY * BLOCK
STEPS = 3
PHASES = STEPS * OWN
D = 4096
COLS = D // (NX * NZ)
PART = 4
SIDE = D // (NX * PART)
CHUNK = NX * SIDE
PAIR = SIDE // COLS
TILES = COLS // 128
SRC = NX * NZ
PAD = 256
PEERS = NY * NX - 1
SENT = CHUNK * PEERS // (PEERS + 1)


def rem(a, n):
    return lax.rem(a, n)


def at(start, size):
    return pl.ds(pl.multiple_of(start, size), size)


def kernel(
    start_hbm, slw_hbm, noise_hbm, w1_ref, w2_ref, w3_ref,
    out_ref, lw_ref, lr_ref,
    start_ref, slw_ref, noise_ref,
    w, s_all, g_all, rx, zs, zx, zown, state, acc, fac, esum,
    ipack, iall, conv, wide, dpack, dall, fsend, fall, e1, ex, e2, ez, e3, el,
    insem, wsem, agx, agz, rxs, zxs, one, snd, sndg,
):
    z, y, xh, xl, core = (lax.axis_index(name) for name in AXES)
    width = w1_ref.shape[0]
    rows_y = at(y * BLOCK, BLOCK)
    side = at(xh * SIDE, SIDE)
    slot = xh * NZ + z

    def zpeer(dz):
        return (rem(z + dz, NZ), y, xh, xl, core)

    def xypeer(rel):
        dy, dx = divmod(rel, NX)
        return (z, rem(y + dy, NY), rem(xh + dx, NX), rem(xl + dx, NX), core)

    def zxpeer(k):
        dz, dx = divmod(k, NX)
        return (rem(z + dz, NZ), y, rem(xh + dx, NX), rem(xl + dx, NX), core)

    def gpeer(k):
        dl, dc = divmod(k, 2)
        return (z, y, xh, rem(xl + dl, 2), rem(core + dc, 2))

    def push(src, dst, send, recv, to):
        pltpu.make_async_remote_copy(
            src_ref=src, dst_ref=dst, send_sem=send, recv_sem=recv, device_id=to, device_id_type=MESH
        ).start()

    def arrived(ref, recv):
        pltpu.make_async_remote_copy(
            src_ref=ref, dst_ref=ref, send_sem=snd.at[0], recv_sem=recv,
            device_id=zpeer(1), device_id_type=MESH,
        ).wait_recv()

    def left(ref, send):
        pltpu.make_async_remote_copy(
            src_ref=ref, dst_ref=ref, send_sem=send, recv_sem=one.at[0],
            device_id=zpeer(1), device_id_type=MESH,
        ).wait_send()

    inputs = (
        pltpu.make_async_copy(start_hbm, start_ref, insem.at[0]),
        pltpu.make_async_copy(noise_hbm, noise_ref, insem.at[1]),
        pltpu.make_async_copy(slw_hbm, slw_ref, insem.at[2]),
    )
    for copy in inputs:
        copy.start()

    barrier = pltpu.get_barrier_semaphore()
    greeted = (
        [zxpeer(k) for k in range(1, SRC)]
        + [xypeer(r) for r in range(2, PEERS + 1)]
        + [gpeer(k) for k in range(1, 4)]
    )
    for to in greeted:
        pl.semaphore_signal(barrier, inc=1, device_id=to, device_id_type=MESH)

    weights = (w1_ref, w2_ref, w3_ref)

    def weight_copy(m, k, half):
        return pltpu.make_async_copy(
            weights[k].at[:, at(half * (D // NX) + m * SIDE, SIDE)],
            w.at[m, k, pl.ds(0, width), pl.ds(half * SIDE, SIDE)],
            wsem.at[m, k, half],
        )

    @pl.loop(0, PART)
    def _(m):
        for k in range(3):
            for half in range(NX):
                weight_copy(m, k, half).start()

    per_side = D // NX // 128
    inputs[0].wait()
    for t in range(D // 128):
        v = start_ref[:, t * 128 : (t + 1) * 128]
        xs, tl = divmod(t, per_side)
        for i in range(OWN):
            ipack[xs, i, tl : tl + 1, :] = v[i : i + 1]
            r = i * TILES + tl % TILES
            dpack[xs * NZ + tl // TILES, r : r + 1, :] = v[i : i + 1]
    for i in range(OWN):
        conv[i] = ipack[:, i].astype(BF16)
        iall[i, slot] = conv[i, xh]

    pl.semaphore_wait(barrier, len(greeted))

    for i in range(OWN):
        for k in range(1, SRC):
            to = zxpeer(k)
            push(conv.at[i, to[2]], iall.at[i, slot], snd.at[0], one.at[6 + i], to)

    inputs[1].wait()
    for k in range(STEPS):
        for t in range(D // 128):
            v = noise_ref[k, :, t * 128 : (t + 1) * 128].astype(F32)
            xs, tl = divmod(t, per_side)
            for i in range(OWN):
                r = (k + 1) * OWN * TILES + i * TILES + tl % TILES
                dpack[xs * NZ + tl // TILES, r : r + 1, :] = v[i : i + 1]
    dall[at(slot * 16, 16), :] = dpack[slot]
    for k in range(1, SRC):
        to = zxpeer(k)
        push(dpack.at[to[2] * NZ + to[0]], dall.at[at(slot * 16, 16), :], snd.at[1], one.at[1], to)

    @pl.loop(0, PART)
    def _(m):
        for k in range(3):
            w[m, k, width:PAD, :] = jnp.zeros((PAD - width, CHUNK), BF16)

    esum[...] = jnp.zeros_like(esum)
    fsend[...] = jnp.zeros_like(fsend)

    def spread(p, m):
        for rel in range(1, PEERS + 1):
            block = s_all.at[p, m, rows_y, side]
            push(block, block, snd.at[2], agx.at[p, m], xypeer(rel))

    def forward(p, m):
        arrived(s_all.at[p, m, :, pl.ds(0, SENT)], agx.at[p, m])
        term = lax.dot_general(
            w[m].reshape(3 * PAD, CHUNK), s_all[p, m], (((1,), (1,)), ((), ())), preferred_element_type=F32
        )

        @pl.when(m == 0)
        def _():
            acc[...] = term

        @pl.when(m != 0)
        def _():
            acc[...] += term

    def gathered(ref, row, stride):
        lo = ref[pl.ds(row, NZ, stride=stride), :]
        hi = ref[pl.ds(NZ * stride + row, NZ, stride=stride), :]
        return jnp.concatenate([lo, hi], axis=0)

    for i in range(OWN):
        arrived(iall.at[i, pl.ds(0, SRC - 1)], one.at[6 + i])
        wide[...] = iall[i].reshape(SRC * per_side, 128).astype(F32)
        for tl in range(per_side):
            m, pos = divmod(tl, SIDE // 128)
            lanes = at(xh * SIDE + pos * 128, 128)
            s_all[i, m, rows_y, lanes] = gathered(wide, tl, per_side).astype(BF16)
            if pos == SIDE // 128 - 1:
                spread(i, m)

    arrived(dall.at[pl.ds(0, 16 * (SRC - 1)), :], one.at[1])
    for i in range(OWN):
        for tt in range(TILES):
            state[i, :, tt * 128 : (tt + 1) * 128] = gathered(dall, i * TILES + tt, 16)

    @pl.loop(0, PART)
    def _(m):
        for k in range(3):
            for half in range(NX):
                weight_copy(m, k, half).wait()
        forward(0, m)

    def factors(p):
        h = rem(p, OWN)

        def part(q, total):
            r = q * 64
            pa, pb, pc = (acc[at(k * PAD + r, 64), :] for k in range(3))
            e = jnp.exp(-jnp.abs(pa))
            soft = jnp.maximum(pa, 0.0) + jnp.log1p(e)
            inv = 1.0 / (1.0 + e)
            sig = jnp.where(pa >= 0, inv, e * inv)
            tan = jnp.tanh(pb)
            st = soft * tan
            fac[at(r, 64), :] = (sig * tan * pc).astype(BF16)
            fac[at(PAD + r, 64), :] = (soft * (1.0 - tan * tan) * pc).astype(BF16)
            fac[at(2 * PAD + r, 64), :] = st.astype(BF16)
            return total + jnp.sum(st * pc, axis=0, keepdims=True)

        total = lax.fori_loop(0, PAD // 64, part, jnp.zeros((1, ROWS), F32))
        esum[pl.ds(h, 1), 0:ROWS] += total

    def backward(p):
        factors(p)

        @pl.loop(0, PART)
        def _(m):
            g = lax.dot_general(
                fac[...], w[m].reshape(3 * PAD, CHUNK), (((0,), (0,)), ((), ())), preferred_element_type=F32
            )
            g_all[p, m] = g.astype(BF16)
            for rel in range(1, PEERS + 1):
                to = xypeer(rel)
                block = g_all.at[p, m, at(to[1] * BLOCK, BLOCK), at(to[2] * SIDE, SIDE)]
                push(block, rx.at[p, m, rel - 1], sndg.at[p], rxs.at[p, m], to)

    def plane_sum(p, m):
        arrived(rx.at[p, m], rxs.at[p, m])
        total = g_all[p, m, rows_y, side].astype(F32)
        for k in range(PEERS):
            total = total + rx[p, m, k].astype(F32)
        zs[p, m] = total.astype(BF16)
        for jj in range(PAIR):
            j = m * PAIR + jj

            @pl.when(j == z)
            def _():
                zown[...] = total[:, jj * COLS : (jj + 1) * COLS]

            @pl.when(j != z)
            def _():
                dz = rem(j - z + NZ, NZ)
                push(
                    zs.at[p, m, :, pl.ds(jj * COLS, COLS)], zx.at[p, dz - 1], snd.at[3], zxs.at[p],
                    (j, y, xh, xl, core),
                )

    def update(p, n, h):
        arrived(zx.at[p], zxs.at[p])
        grad = zown[...]
        for k in range(NZ - 1):
            grad = grad + zx[p, k].astype(F32)
        beta = jnp.asarray(n + 1, jnp.int32).astype(F32) / STEPS
        for tt in range(TILES):
            cols = slice(tt * 128, (tt + 1) * 128)
            extra = gathered(dall, ((n + 1) * OWN + h) * TILES + tt, 16)
            old = state[h, :, cols]
            state[h, :, cols] = old - 0.05 * (old + beta * grad[:, cols]) + math.sqrt(0.1) * extra

    own_lanes = at(xh * SIDE + rem(z, PAIR) * COLS, COLS)

    def step_on(p):
        n, h = p // OWN, rem(p, OWN)
        update(p, n, h)

        @pl.when(n < STEPS - 1)
        def _():
            block = s_all.at[p + OWN, z // PAIR, rows_y, own_lanes]
            block[...] = state[h].astype(BF16)
            for dz in range(1, NZ):
                push(block, block, snd.at[4], agz.at[p, z], zpeer(dz))

    def pass_on(p, m):
        for jj in range(PAIR):
            j = m * PAIR + jj

            @pl.when(j != z)
            def _():
                arrived(s_all.at[p + OWN, m, rows_y, at(xh * SIDE + jj * COLS, COLS)], agz.at[p, j])

        spread(p + OWN, m)

    early = z < NZ // 2

    def phase(p, carry):
        backward(p)

        @pl.when(p > 0)
        def _():
            @pl.when(jnp.logical_not(early))
            def _():
                step_on(p - 1)

            @pl.loop(0, PART)
            def _(m):
                pass_on(p - 1, m)

        @pl.loop(0, PART)
        def _(m):
            plane_sum(p, m)
            forward(p + 1, m)

        @pl.when(early)
        def _():
            step_on(p)

        return carry

    lax.fori_loop(0, PHASES - 1, phase, 0)

    row = lax.broadcasted_iota(jnp.int32, (8, 128), 0)
    lane = lax.broadcasted_iota(jnp.int32, (8, 128), 1)
    own_lane = y * BLOCK + slot

    last = PHASES - 1
    backward(last)

    inputs[2].wait()
    v = esum[...] / STEPS
    for i in range(OWN):
        v = v - jnp.where((row == i) & (lane == own_lane), slw_ref[i], 0.0)
    e1[...] = v
    for rel in range(1, PEERS + 1):
        push(e1, ex.at[rel - 1], snd.at[5], one.at[3], xypeer(rel))

    @pl.when(jnp.logical_not(early))
    def _():
        update(last - 1, STEPS - 1, 0)

    @pl.loop(0, PART)
    def _(m):
        plane_sum(last, m)

    arrived(ex, one.at[3])
    total = e1[...]
    for k in range(PEERS):
        total = total + ex[k]
    e2[...] = total
    for dz in range(1, NZ):
        push(e2, ez.at[dz - 1], snd.at[6], one.at[4], zpeer(dz))

    update(last, STEPS - 1, 1)
    for i in range(OWN):
        for tt in range(TILES):
            tile = state[i, :, tt * 128 : (tt + 1) * 128]
            fsend[pl.ds(i * TILES + tt, NZ, stride=8), :] = tile[0:NZ]
            fsend[pl.ds(NZ * 8 + i * TILES + tt, NZ, stride=8), :] = tile[NZ:]
    for k in range(1, SRC):
        to = zxpeer(k)
        push(fsend.at[at((to[2] * NZ + to[0]) * 8, 8), :], fall.at[slot], snd.at[8], one.at[2], to)
    fall[slot] = fsend[at(slot * 8, 8), :]

    arrived(ez, one.at[4])
    total = e2[...]
    for k in range(NZ - 1):
        total = total + ez[k]
    e3[...] = -total
    for k in range(1, 4):
        push(e3, el.at[k - 1], snd.at[7], one.at[5], gpeer(k))
    for i in range(OWN):
        lw_ref[i] = jnp.sum(jnp.where((row == i) & (lane == own_lane), -total, 0.0))
    arrived(el, one.at[5])
    used = (row < OWN) & (lane < ROWS)
    lws = [jnp.where(used, v, -jnp.inf) for v in [-total] + [el[k] for k in range(3)]]
    top = jnp.max(jnp.maximum(jnp.maximum(lws[0], lws[1]), jnp.maximum(lws[2], lws[3])))
    mass = jnp.sum(sum(jnp.exp(v - top) for v in lws))
    lr_ref[0] = jnp.max(top + jnp.log(jnp.full((8, 128), mass, F32)) - math.log(4 * OWN * ROWS))

    arrived(fall.at[pl.ds(0, SRC - 1)], one.at[2])
    for src in range(SRC):
        for i in range(OWN):
            for tt in range(TILES):
                c = (src * TILES + tt) * 128
                out_ref[i : i + 1, c : c + 128] = fall[src, i * TILES + tt : i * TILES + tt + 1, :]

    left(iall.at[:, pl.ds(0, SRC - 1)], snd.at[0])
    left(dpack.at[pl.ds(0, SRC - 1)], snd.at[1])
    left(s_all.at[:, :, :, pl.ds(0, SENT)], snd.at[2])
    left(zx, snd.at[3])
    left(zx.at[pl.ds(0, PHASES - OWN)], snd.at[4])
    left(ex, snd.at[5])
    left(ez, snd.at[6])
    left(el, snd.at[7])
    left(fall.at[pl.ds(0, SRC - 1)], snd.at[8])
    for p in range(PHASES):
        left(g_all.at[p, :, :, pl.ds(0, SENT)], sndg.at[p])


def per_device(start_state, start_log_weight, noise, first_weight, second_weight, third_weight):
    smem = pl.BlockSpec(memory_space=pltpu.SMEM)
    hbm = pl.BlockSpec(memory_space=pl.ANY)
    tile = (8, 128)
    state, log_weight, log_ratio = pl.pallas_call(
        kernel,
        out_shape=(
            jax.ShapeDtypeStruct((OWN, D), F32),
            jax.ShapeDtypeStruct((OWN,), F32),
            jax.ShapeDtypeStruct((1,), F32),
        ),
        in_specs=[hbm] * 6,
        out_specs=(pl.BlockSpec(memory_space=pltpu.VMEM), smem, smem),
        scratch_shapes=[
            pltpu.VMEM((OWN, D), F32),
            pltpu.SMEM((OWN,), F32),
            pltpu.VMEM((STEPS, OWN, D), BF16),
            pltpu.VMEM((PART, 3, PAD, CHUNK), BF16),
            pltpu.VMEM((PHASES, PART, ROWS, CHUNK), BF16),
            pltpu.VMEM((PHASES, PART, ROWS, CHUNK), BF16),
            pltpu.VMEM((PHASES, PART, PEERS, BLOCK, SIDE), BF16),
            pltpu.VMEM((PHASES, PART, BLOCK, SIDE), BF16),
            pltpu.VMEM((PHASES, NZ - 1, BLOCK, COLS), BF16),
            pltpu.VMEM((BLOCK, COLS), F32),
            pltpu.VMEM((OWN, BLOCK, COLS), F32),
            pltpu.VMEM((3 * PAD, ROWS), F32),
            pltpu.VMEM((3 * PAD, ROWS), BF16),
            pltpu.VMEM(tile, F32),
            pltpu.VMEM((NX, OWN, 16, 128), F32),
            pltpu.VMEM((OWN, SRC, 16, 128), BF16),
            pltpu.VMEM((OWN, NX, 16, 128), BF16),
            pltpu.VMEM((SRC * 16, 128), F32),
            pltpu.VMEM((SRC, 16, 128), F32),
            pltpu.VMEM((SRC * 16, 128), F32),
            pltpu.VMEM((SRC * 8, 128), F32),
            pltpu.VMEM((SRC, 8, 128), F32),
            pltpu.VMEM(tile, F32),
            pltpu.VMEM((PEERS, *tile), F32),
            pltpu.VMEM(tile, F32),
            pltpu.VMEM((NZ - 1, *tile), F32),
            pltpu.VMEM(tile, F32),
            pltpu.VMEM((3, *tile), F32),
            pltpu.SemaphoreType.DMA((3,)),
            pltpu.SemaphoreType.DMA((PART, 3, NX)),
            pltpu.SemaphoreType.DMA((PHASES, PART)),
            pltpu.SemaphoreType.DMA((PHASES - OWN, NZ)),
            pltpu.SemaphoreType.DMA((PHASES, PART)),
            pltpu.SemaphoreType.DMA((PHASES,)),
            pltpu.SemaphoreType.DMA((8,)),
            pltpu.SemaphoreType.DMA((9,)),
            pltpu.SemaphoreType.DMA((PHASES,)),
        ],
        compiler_params=pltpu.CompilerParams(
            collective_id=0, has_side_effects=True, vmem_limit_bytes=67043328
        ),
    )(start_state, start_log_weight, noise, first_weight, second_weight, third_weight)
    return state, log_weight, log_ratio[0]


def solution(mesh):
    torus = Mesh(mesh.devices.reshape(8, 4, 2, 2, 2), AXES)
    placed = (
        P(BLK_GRP, None),
        P(BLK_GRP),
        P(None, BLK_GRP, None),
        P(BLK, None),
        P(BLK, None),
        P(BLK, None),
    )
    return jax.shard_map(
        per_device,
        mesh=torus,
        in_specs=placed,
        out_specs=(P(BLK_GRP, None), P(BLK_GRP), P()),
        check_vma=False,
    )
```

```python
import math

import jax
import jax.numpy as jnp
from jax import lax
from jax.experimental import pallas as pl
from jax.experimental.pallas import tpu as pltpu
from jax.sharding import Mesh
from jax.sharding import PartitionSpec as P

BLK = ("blk_0", "blk_1", "blk_2")
BLK_GRP = ("blk_0", "blk_1", "blk_2", "grp_0", "grp_1")
AXES = BLK_GRP
MESH = pl.DeviceIdType.MESH
F32 = jnp.float32
BF16 = jnp.bfloat16

NZ, NY, NX = 8, 4, 2
OWN = 2
BLOCK = NX * NZ
ROWS = NY * BLOCK
STEPS = 3
PHASES = STEPS * OWN
D = 4096
COLS = D // (NX * NZ)
PART = 4
SIDE = D // (NX * PART)
CHUNK = NX * SIDE
PAIR = SIDE // COLS
TILES = COLS // 128
SRC = NX * NZ
PAD = 256
PEERS = NY * NX - 1
SENT = CHUNK * PEERS // (PEERS + 1)


def rem(a, n):
    return lax.rem(a, n)


def at(start, size):
    return pl.ds(pl.multiple_of(start, size), size)


def kernel(
    start_hbm, slw_hbm, noise_hbm, w1_ref, w2_ref, w3_ref,
    out_ref, lw_ref, lr_ref,
    start_ref, slw_ref, noise_ref,
    w, s_all, g_all, rx, zs, zx, zown, state, acc, fac, esum,
    ipack, iall, conv, wide, dpack, dall, fsend, fall, hsend, hall, e1, ex, e2, ez, e3, el,
    insem, wsem, agx, agz, rxs, zxs, hsem, one, snd, sndg,
):
    z, y, xh, xl, core = (lax.axis_index(name) for name in AXES)
    width = w1_ref.shape[0]
    rows_y = at(y * BLOCK, BLOCK)
    side = at(xh * SIDE, SIDE)
    slot = xh * NZ + z

    def zpeer(dz):
        return (rem(z + dz, NZ), y, xh, xl, core)

    def xypeer(rel):
        dy, dx = divmod(rel, NX)
        return (z, rem(y + dy, NY), rem(xh + dx, NX), rem(xl + dx, NX), core)

    def zxpeer(k):
        dz, dx = divmod(k, NX)
        return (rem(z + dz, NZ), y, rem(xh + dx, NX), rem(xl + dx, NX), core)

    def gpeer(k):
        dl, dc = divmod(k, 2)
        return (z, y, xh, rem(xl + dl, 2), rem(core + dc, 2))

    def push(src, dst, send, recv, to):
        pltpu.make_async_remote_copy(
            src_ref=src, dst_ref=dst, send_sem=send, recv_sem=recv, device_id=to, device_id_type=MESH
        ).start()

    def arrived(ref, recv):
        pltpu.make_async_remote_copy(
            src_ref=ref, dst_ref=ref, send_sem=snd.at[0], recv_sem=recv,
            device_id=zpeer(1), device_id_type=MESH,
        ).wait_recv()

    def left(ref, send):
        pltpu.make_async_remote_copy(
            src_ref=ref, dst_ref=ref, send_sem=send, recv_sem=one.at[0],
            device_id=zpeer(1), device_id_type=MESH,
        ).wait_send()

    inputs = (
        pltpu.make_async_copy(start_hbm, start_ref, insem.at[0]),
        pltpu.make_async_copy(noise_hbm, noise_ref, insem.at[1]),
        pltpu.make_async_copy(slw_hbm, slw_ref, insem.at[2]),
    )
    for copy in inputs:
        copy.start()

    barrier = pltpu.get_barrier_semaphore()
    greeted = (
        [zxpeer(k) for k in range(1, SRC)]
        + [xypeer(r) for r in range(2, PEERS + 1)]
        + [gpeer(k) for k in range(1, 4)]
    )
    for to in greeted:
        pl.semaphore_signal(barrier, inc=1, device_id=to, device_id_type=MESH)

    weights = (w1_ref, w2_ref, w3_ref)

    def weight_copy(m, k, half):
        return pltpu.make_async_copy(
            weights[k].at[:, at(half * (D // NX) + m * SIDE, SIDE)],
            w.at[m, k, pl.ds(0, width), pl.ds(half * SIDE, SIDE)],
            wsem.at[m, k, half],
        )

    @pl.loop(0, PART)
    def _(m):
        for k in range(3):
            for half in range(NX):
                weight_copy(m, k, half).start()

    per_side = D // NX // 128
    inputs[0].wait()
    for t in range(D // 128):
        v = start_ref[:, t * 128 : (t + 1) * 128]
        xs, tl = divmod(t, per_side)
        for i in range(OWN):
            ipack[xs, i, tl : tl + 1, :] = v[i : i + 1]
            r = i * TILES + tl % TILES
            dpack[xs * NZ + tl // TILES, r : r + 1, :] = v[i : i + 1]
    for i in range(OWN):
        conv[i] = ipack[:, i].astype(BF16)
        iall[i, slot] = conv[i, xh]

    pl.semaphore_wait(barrier, len(greeted))

    for i in range(OWN):
        for k in range(1, SRC):
            to = zxpeer(k)
            push(conv.at[i, to[2]], iall.at[i, slot], snd.at[0], one.at[6 + i], to)

    inputs[1].wait()
    for k in range(STEPS):
        for t in range(D // 128):
            v = noise_ref[k, :, t * 128 : (t + 1) * 128].astype(F32)
            xs, tl = divmod(t, per_side)
            for i in range(OWN):
                r = (k + 1) * OWN * TILES + i * TILES + tl % TILES
                dpack[xs * NZ + tl // TILES, r : r + 1, :] = v[i : i + 1]
    dall[at(slot * 16, 16), :] = dpack[slot]
    for k in range(1, SRC):
        to = zxpeer(k)
        push(dpack.at[to[2] * NZ + to[0]], dall.at[at(slot * 16, 16), :], snd.at[1], one.at[1], to)

    @pl.loop(0, PART)
    def _(m):
        for k in range(3):
            w[m, k, width:PAD, :] = jnp.zeros((PAD - width, CHUNK), BF16)

    esum[...] = jnp.zeros_like(esum)
    fsend[...] = jnp.zeros_like(fsend)

    def spread(p, m):
        for rel in range(1, PEERS + 1):
            block = s_all.at[p, m, rows_y, side]
            push(block, block, snd.at[2], agx.at[p, m], xypeer(rel))

    def forward(p, m):
        arrived(s_all.at[p, m, :, pl.ds(0, SENT)], agx.at[p, m])
        term = lax.dot_general(
            w[m].reshape(3 * PAD, CHUNK), s_all[p, m], (((1,), (1,)), ((), ())), preferred_element_type=F32
        )

        @pl.when(m == 0)
        def _():
            acc[...] = term

        @pl.when(m != 0)
        def _():
            acc[...] += term

    def gathered(ref, row, stride):
        lo = ref[pl.ds(row, NZ, stride=stride), :]
        hi = ref[pl.ds(NZ * stride + row, NZ, stride=stride), :]
        return jnp.concatenate([lo, hi], axis=0)

    for i in range(OWN):
        arrived(iall.at[i, pl.ds(0, SRC - 1)], one.at[6 + i])
        wide[...] = iall[i].reshape(SRC * per_side, 128).astype(F32)
        for tl in range(per_side):
            m, pos = divmod(tl, SIDE // 128)
            lanes = at(xh * SIDE + pos * 128, 128)
            s_all[i, m, rows_y, lanes] = gathered(wide, tl, per_side).astype(BF16)
            if pos == SIDE // 128 - 1:
                spread(i, m)

    arrived(dall.at[pl.ds(0, 16 * (SRC - 1)), :], one.at[1])
    for i in range(OWN):
        for tt in range(TILES):
            state[i, :, tt * 128 : (tt + 1) * 128] = gathered(dall, i * TILES + tt, 16)

    @pl.loop(0, PART)
    def _(m):
        for k in range(3):
            for half in range(NX):
                weight_copy(m, k, half).wait()
        forward(0, m)

    def factors(p):
        h = rem(p, OWN)

        def part(q, total):
            r = q * 64
            pa, pb, pc = (acc[at(k * PAD + r, 64), :] for k in range(3))
            e = jnp.exp(-jnp.abs(pa))
            soft = jnp.maximum(pa, 0.0) + jnp.log1p(e)
            inv = 1.0 / (1.0 + e)
            sig = jnp.where(pa >= 0, inv, e * inv)
            tan = jnp.tanh(pb)
            st = soft * tan
            fac[at(r, 64), :] = (sig * tan * pc).astype(BF16)
            fac[at(PAD + r, 64), :] = (soft * (1.0 - tan * tan) * pc).astype(BF16)
            fac[at(2 * PAD + r, 64), :] = st.astype(BF16)
            return total + jnp.sum(st * pc, axis=0, keepdims=True)

        total = lax.fori_loop(0, PAD // 64, part, jnp.zeros((1, ROWS), F32))
        esum[pl.ds(h, 1), 0:ROWS] += total

    def backward(p, first, end):
        @pl.loop(first, end)
        def _(m):
            g = lax.dot_general(
                fac[...], w[m].reshape(3 * PAD, CHUNK), (((0,), (0,)), ((), ())), preferred_element_type=F32
            )
            g_all[p, m] = g.astype(BF16)
            for rel in range(1, PEERS + 1):
                to = xypeer(rel)
                block = g_all.at[p, m, at(to[1] * BLOCK, BLOCK), at(to[2] * SIDE, SIDE)]
                push(block, rx.at[p, m, rel - 1], sndg.at[p], rxs.at[p, m], to)

    def plane_total(p, m):
        arrived(rx.at[p, m], rxs.at[p, m])
        total = g_all[p, m, rows_y, side].astype(F32)
        for k in range(PEERS):
            total = total + rx[p, m, k].astype(F32)
        return total

    def plane_sum(p, m):
        total = plane_total(p, m)
        zs[p, m] = total.astype(BF16)
        for jj in range(PAIR):
            j = m * PAIR + jj

            @pl.when(j == z)
            def _():
                zown[...] = total[:, jj * COLS : (jj + 1) * COLS]

            @pl.when(j != z)
            def _():
                dz = rem(j - z + NZ, NZ)
                push(
                    zs.at[p, m, :, pl.ds(jj * COLS, COLS)], zx.at[p, dz - 1], snd.at[3], zxs.at[p],
                    (j, y, xh, xl, core),
                )

    def update(p, n, h):
        arrived(zx.at[p], zxs.at[p])
        grad = zown[...]
        for k in range(NZ - 1):
            grad = grad + zx[p, k].astype(F32)
        beta = jnp.asarray(n + 1, jnp.int32).astype(F32) / STEPS
        for tt in range(TILES):
            cols = slice(tt * 128, (tt + 1) * 128)
            extra = gathered(dall, ((n + 1) * OWN + h) * TILES + tt, 16)
            old = state[h, :, cols]
            state[h, :, cols] = old - 0.05 * (old + beta * grad[:, cols]) + math.sqrt(0.1) * extra

    own_lanes = at(xh * SIDE + rem(z, PAIR) * COLS, COLS)

    def step_on(p):
        n, h = p // OWN, rem(p, OWN)
        update(p, n, h)
        block = s_all.at[p + OWN, z // PAIR, rows_y, own_lanes]
        block[...] = state[h].astype(BF16)
        for dz in range(1, NZ):
            push(block, block, snd.at[4], agz.at[p, z], zpeer(dz))

        @pl.when(n == STEPS - 2)
        def _():
            base = h * SRC * 8
            for tt in range(TILES):
                tile = state[h, :, tt * 128 : (tt + 1) * 128]
                fsend[pl.ds(base + tt, NZ, stride=8), :] = tile[0:NZ]
                fsend[pl.ds(base + NZ * 8 + tt, NZ, stride=8), :] = tile[NZ:]
            for k in range(1, SRC):
                to = zxpeer(k)
                push(
                    fsend.at[at(base + (to[2] * NZ + to[0]) * 8, 8), :], fall.at[h, slot],
                    snd.at[8], one.at[2], to,
                )
            fall[h, slot] = fsend[at(base + slot * 8, 8), :]

    def pass_on(p, m):
        for jj in range(PAIR):
            j = m * PAIR + jj

            @pl.when(j != z)
            def _():
                arrived(s_all.at[p + OWN, m, rows_y, at(xh * SIDE + jj * COLS, COLS)], agz.at[p, j])

        spread(p + OWN, m)

    early = z < NZ // 2

    half = PART // 2

    def phase(p, carry):
        factors(p)
        backward(p, 0, half)

        @pl.when((p > 0) & jnp.logical_not(early))
        def _():
            step_on(p - 1)

        backward(p, half, PART)

        @pl.when(p > 0)
        def _():
            @pl.loop(0, PART)
            def _(m):
                pass_on(p - 1, m)

        @pl.loop(0, PART)
        def _(m):
            plane_sum(p, m)

        @pl.loop(0, PART)
        def _(m):
            forward(p + 1, m)

        @pl.when(early)
        def _():
            step_on(p)

        return carry

    lax.fori_loop(0, PHASES - OWN, phase, 0)

    def home_sum(h, pair):
        base = (h * 2 + pair) * SRC * 8

        @pl.loop(0, PART // 2)
        def _(q):
            total = plane_total(PHASES - OWN + h, pair * (PART // 2) + q)
            for pos in range(SIDE // 128):
                tile = total[:, pos * 128 : (pos + 1) * 128]
                r = base + q * (SIDE // 128) + pos
                hsend[pl.ds(r, NZ, stride=8), :] = tile[0:NZ]
                hsend[pl.ds(r + NZ * 8, NZ, stride=8), :] = tile[NZ:]

        for k in range(1, SRC):
            to = zxpeer(k)
            push(
                hsend.at[at(base + (to[2] * NZ + to[0]) * 8, 8), :], hall.at[h, pair, slot],
                snd.at[9], hsem.at[h], to,
            )
        hall[h, pair, slot] = hsend[at(base + slot * 8, 8), :]

    def home_base():
        arrived(fall.at[:, pl.ds(0, SRC - 1)], one.at[2])
        for src in range(SRC):
            for tt in range(TILES):
                c = (src * TILES + tt) * 128
                extra = noise_ref[STEPS - 1, :, c : c + 128].astype(F32)
                for i in range(OWN):
                    old = fall[i, src, tt : tt + 1, :]
                    out_ref[i : i + 1, c : c + 128] = old - 0.05 * old + math.sqrt(0.1) * extra[i : i + 1]

    def home_end(h):
        arrived(hall.at[h, :, pl.ds(0, SRC - 1)], hsem.at[h])
        for xs in range(NX):
            for pair in range(2):
                grad = hall[h, pair, xs * NZ]
                for k in range(1, NZ):
                    grad = grad + hall[h, pair, xs * NZ + k]
                grad = 0.05 * grad
                for r in range(8):
                    c = (xs * per_side + pair * 8 + r) * 128
                    out_ref[h : h + 1, c : c + 128] -= grad[r : r + 1]

    p = PHASES - OWN
    factors(p)
    backward(p, 0, half)

    @pl.when(jnp.logical_not(early))
    def _():
        step_on(p - 1)

    backward(p, half, PART)

    @pl.loop(0, PART)
    def _(m):
        pass_on(p - 1, m)

    home_sum(0, 0)
    home_sum(0, 1)

    @pl.loop(0, PART)
    def _(m):
        forward(p + 1, m)

    row = lax.broadcasted_iota(jnp.int32, (8, 128), 0)
    lane = lax.broadcasted_iota(jnp.int32, (8, 128), 1)
    own_lane = y * BLOCK + slot

    factors(p + 1)
    backward(p + 1, 0, PART)

    inputs[2].wait()
    v = esum[...] / STEPS
    for i in range(OWN):
        v = v - jnp.where((row == i) & (lane == own_lane), slw_ref[i], 0.0)
    e1[...] = v
    for rel in range(1, PEERS + 1):
        push(e1, ex.at[rel - 1], snd.at[5], one.at[3], xypeer(rel))

    home_base()
    home_end(0)
    home_sum(1, 0)

    arrived(ex, one.at[3])
    total = e1[...]
    for k in range(PEERS):
        total = total + ex[k]
    e2[...] = total
    for dz in range(1, NZ):
        push(e2, ez.at[dz - 1], snd.at[6], one.at[4], zpeer(dz))

    home_sum(1, 1)

    arrived(ez, one.at[4])
    total = e2[...]
    for k in range(NZ - 1):
        total = total + ez[k]
    e3[...] = -total
    for k in range(1, 4):
        push(e3, el.at[k - 1], snd.at[7], one.at[5], gpeer(k))
    for i in range(OWN):
        lw_ref[i] = jnp.sum(jnp.where((row == i) & (lane == own_lane), -total, 0.0))
    arrived(el, one.at[5])
    used = (row < OWN) & (lane < ROWS)
    lws = [jnp.where(used, v, -jnp.inf) for v in [-total] + [el[k] for k in range(3)]]
    top = jnp.max(jnp.maximum(jnp.maximum(lws[0], lws[1]), jnp.maximum(lws[2], lws[3])))
    mass = jnp.sum(sum(jnp.exp(v - top) for v in lws))
    lr_ref[0] = jnp.max(top + jnp.log(jnp.full((8, 128), mass, F32)) - math.log(4 * OWN * ROWS))

    home_end(1)

    left(iall.at[:, pl.ds(0, SRC - 1)], snd.at[0])
    left(dpack.at[pl.ds(0, SRC - 1)], snd.at[1])
    left(s_all.at[:, :, :, pl.ds(0, SENT)], snd.at[2])
    left(zx, snd.at[3])
    left(zx, snd.at[4])
    left(ex, snd.at[5])
    left(ez, snd.at[6])
    left(el, snd.at[7])
    left(fall.at[:, pl.ds(0, SRC - 1)], snd.at[8])
    left(hall.at[:, :, pl.ds(0, SRC - 1)], snd.at[9])
    for p in range(PHASES):
        left(g_all.at[p, :, :, pl.ds(0, SENT)], sndg.at[p])


def per_device(start_state, start_log_weight, noise, first_weight, second_weight, third_weight):
    smem = pl.BlockSpec(memory_space=pltpu.SMEM)
    hbm = pl.BlockSpec(memory_space=pl.ANY)
    tile = (8, 128)
    state, log_weight, log_ratio = pl.pallas_call(
        kernel,
        out_shape=(
            jax.ShapeDtypeStruct((OWN, D), F32),
            jax.ShapeDtypeStruct((OWN,), F32),
            jax.ShapeDtypeStruct((1,), F32),
        ),
        in_specs=[hbm] * 6,
        out_specs=(pl.BlockSpec(memory_space=pltpu.VMEM), smem, smem),
        scratch_shapes=[
            pltpu.VMEM((OWN, D), F32),
            pltpu.SMEM((OWN,), F32),
            pltpu.VMEM((STEPS, OWN, D), BF16),
            pltpu.VMEM((PART, 3, PAD, CHUNK), BF16),
            pltpu.VMEM((PHASES, PART, ROWS, CHUNK), BF16),
            pltpu.VMEM((PHASES, PART, ROWS, CHUNK), BF16),
            pltpu.VMEM((PHASES, PART, PEERS, BLOCK, SIDE), BF16),
            pltpu.VMEM((PHASES - OWN, PART, BLOCK, SIDE), BF16),
            pltpu.VMEM((PHASES - OWN, NZ - 1, BLOCK, COLS), BF16),
            pltpu.VMEM((BLOCK, COLS), F32),
            pltpu.VMEM((OWN, BLOCK, COLS), F32),
            pltpu.VMEM((3 * PAD, ROWS), F32),
            pltpu.VMEM((3 * PAD, ROWS), BF16),
            pltpu.VMEM(tile, F32),
            pltpu.VMEM((NX, OWN, 16, 128), F32),
            pltpu.VMEM((OWN, SRC, 16, 128), BF16),
            pltpu.VMEM((OWN, NX, 16, 128), BF16),
            pltpu.VMEM((SRC * 16, 128), F32),
            pltpu.VMEM((SRC, 16, 128), F32),
            pltpu.VMEM((SRC * 16, 128), F32),
            pltpu.VMEM((OWN * SRC * 8, 128), F32),
            pltpu.VMEM((OWN, SRC, 8, 128), F32),
            pltpu.VMEM((OWN * 2 * SRC * 8, 128), F32),
            pltpu.VMEM((OWN, 2, SRC, 8, 128), F32),
            pltpu.VMEM(tile, F32),
            pltpu.VMEM((PEERS, *tile), F32),
            pltpu.VMEM(tile, F32),
            pltpu.VMEM((NZ - 1, *tile), F32),
            pltpu.VMEM(tile, F32),
            pltpu.VMEM((3, *tile), F32),
            pltpu.SemaphoreType.DMA((3,)),
            pltpu.SemaphoreType.DMA((PART, 3, NX)),
            pltpu.SemaphoreType.DMA((PHASES, PART)),
            pltpu.SemaphoreType.DMA((PHASES - OWN, NZ)),
            pltpu.SemaphoreType.DMA((PHASES, PART)),
            pltpu.SemaphoreType.DMA((PHASES - OWN,)),
            pltpu.SemaphoreType.DMA((OWN,)),
            pltpu.SemaphoreType.DMA((8,)),
            pltpu.SemaphoreType.DMA((10,)),
            pltpu.SemaphoreType.DMA((PHASES,)),
        ],
        compiler_params=pltpu.CompilerParams(
            collective_id=0, has_side_effects=True, vmem_limit_bytes=67043328
        ),
    )(start_state, start_log_weight, noise, first_weight, second_weight, third_weight)
    return state, log_weight, log_ratio[0]


def solution(mesh):
    torus = Mesh(mesh.devices.reshape(8, 4, 2, 2, 2), AXES)
    placed = (
        P(BLK_GRP, None),
        P(BLK_GRP),
        P(None, BLK_GRP, None),
        P(BLK, None),
        P(BLK, None),
        P(BLK, None),
    )
    return jax.shard_map(
        per_device,
        mesh=torus,
        in_specs=placed,
        out_specs=(P(BLK_GRP, None), P(BLK_GRP), P()),
        check_vma=False,
    )
```

```python
import math

import jax
import jax.numpy as jnp
from jax import lax
from jax.experimental import pallas as pl
from jax.experimental.pallas import tpu as pltpu
from jax.sharding import Mesh
from jax.sharding import PartitionSpec as P

BLK = ("blk_0", "blk_1", "blk_2")
BLK_GRP = ("blk_0", "blk_1", "blk_2", "grp_0", "grp_1")
AXES = BLK_GRP
MESH = pl.DeviceIdType.MESH
F32 = jnp.float32
BF16 = jnp.bfloat16

NZ, NY, NX = 8, 4, 2
OWN = 2
BLOCK = NX * NZ
ROWS = NY * BLOCK
STEPS = 3
PHASES = STEPS * OWN
D = 4096
COLS = D // (NX * NZ)
PART = 4
SIDE = D // (NX * PART)
CHUNK = NX * SIDE
PAIR = SIDE // COLS
TILES = COLS // 128
SRC = NX * NZ
PAD = 256
PEERS = NY * NX - 1
SENT = CHUNK * PEERS // (PEERS + 1)
FAR_XY = (5, 4, 3, 7, 2, 6, 1)
FAR_Z = (4, 3, 5, 2, 6, 1, 7)
FAR_ZX = tuple(NX * dz + 1 for dz in FAR_Z[:3]) + tuple(NX * dz for dz in FAR_Z[:3]) + tuple(
    NX * dz + dx for dz in FAR_Z[3:] for dx in (1, 0)
) + (1,)


def rem(a, n):
    return lax.rem(a, n)


def at(start, size):
    return pl.ds(pl.multiple_of(start, size), size)


def kernel(
    start_hbm, slw_hbm, noise_hbm, w1_ref, w2_ref, w3_ref,
    out_ref, lw_ref, lr_ref,
    start_ref, slw_ref, noise_ref,
    w, s_all, g_all, rx, zs, zx, zown, state, acc, fac, esum,
    ipack, iall, conv, wide, dpack, dall, fsend, fall, e1, ex, e2, ez, e3, el,
    insem, wsem, agx, agz, rxs, zxs, one, snd, sndg,
):
    z, y, xh, xl, core = (lax.axis_index(name) for name in AXES)
    width = w1_ref.shape[0]
    rows_y = at(y * BLOCK, BLOCK)
    side = at(xh * SIDE, SIDE)
    slot = xh * NZ + z

    def zpeer(dz):
        return (rem(z + dz, NZ), y, xh, xl, core)

    def xypeer(rel):
        dy, dx = divmod(rel, NX)
        return (z, rem(y + dy, NY), rem(xh + dx, NX), rem(xl + dx, NX), core)

    def zxpeer(k):
        dz, dx = divmod(k, NX)
        return (rem(z + dz, NZ), y, rem(xh + dx, NX), rem(xl + dx, NX), core)

    def gpeer(k):
        dl, dc = divmod(k, 2)
        return (z, y, xh, rem(xl + dl, 2), rem(core + dc, 2))

    def push(src, dst, send, recv, to):
        pltpu.make_async_remote_copy(
            src_ref=src, dst_ref=dst, send_sem=send, recv_sem=recv, device_id=to, device_id_type=MESH
        ).start()

    def arrived(ref, recv):
        pltpu.make_async_remote_copy(
            src_ref=ref, dst_ref=ref, send_sem=snd.at[0], recv_sem=recv,
            device_id=zpeer(1), device_id_type=MESH,
        ).wait_recv()

    def left(ref, send):
        pltpu.make_async_remote_copy(
            src_ref=ref, dst_ref=ref, send_sem=send, recv_sem=one.at[0],
            device_id=zpeer(1), device_id_type=MESH,
        ).wait_send()

    inputs = (
        pltpu.make_async_copy(start_hbm, start_ref, insem.at[0]),
        pltpu.make_async_copy(noise_hbm, noise_ref, insem.at[1]),
        pltpu.make_async_copy(slw_hbm, slw_ref, insem.at[2]),
    )
    for copy in inputs:
        copy.start()

    barrier = pltpu.get_barrier_semaphore()
    greeted = (
        [zxpeer(k) for k in range(1, SRC)]
        + [xypeer(r) for r in range(2, PEERS + 1)]
        + [gpeer(k) for k in range(1, 4)]
    )
    for to in greeted:
        pl.semaphore_signal(barrier, inc=1, device_id=to, device_id_type=MESH)

    weights = (w1_ref, w2_ref, w3_ref)

    def weight_copy(m, k, half):
        return pltpu.make_async_copy(
            weights[k].at[:, at(half * (D // NX) + m * SIDE, SIDE)],
            w.at[m, k, pl.ds(0, width), pl.ds(half * SIDE, SIDE)],
            wsem.at[m, k, half],
        )

    @pl.loop(0, PART)
    def _(m):
        for k in range(3):
            for half in range(NX):
                weight_copy(m, k, half).start()

    per_side = D // NX // 128
    inputs[0].wait()
    for t in range(D // 128):
        v = start_ref[:, t * 128 : (t + 1) * 128]
        xs, tl = divmod(t, per_side)
        for i in range(OWN):
            ipack[xs, i, tl : tl + 1, :] = v[i : i + 1]
            r = i * TILES + tl % TILES
            dpack[xs * NZ + tl // TILES, r : r + 1, :] = v[i : i + 1]
    for i in range(OWN):
        conv[i] = ipack[:, i].astype(BF16)
        iall[i, slot] = conv[i, xh]

    pl.semaphore_wait(barrier, len(greeted))

    for i in range(OWN):
        for k in FAR_ZX:
            to = zxpeer(k)
            push(conv.at[i, to[2]], iall.at[i, slot], snd.at[0], one.at[6 + i], to)

    inputs[1].wait()
    for k in range(STEPS):
        for t in range(D // 128):
            v = noise_ref[k, :, t * 128 : (t + 1) * 128].astype(F32)
            xs, tl = divmod(t, per_side)
            for i in range(OWN):
                r = (k + 1) * OWN * TILES + i * TILES + tl % TILES
                dpack[xs * NZ + tl // TILES, r : r + 1, :] = v[i : i + 1]
    dall[at(slot * 16, 16), :] = dpack[slot]
    for k in FAR_ZX:
        to = zxpeer(k)
        push(dpack.at[to[2] * NZ + to[0]], dall.at[at(slot * 16, 16), :], snd.at[1], one.at[1], to)

    @pl.loop(0, PART)
    def _(m):
        for k in range(3):
            w[m, k, width:PAD, :] = jnp.zeros((PAD - width, CHUNK), BF16)

    esum[...] = jnp.zeros_like(esum)
    fsend[...] = jnp.zeros_like(fsend)

    def spread(p, m):
        for rel in FAR_XY:
            block = s_all.at[p, m, rows_y, side]
            push(block, block, snd.at[2], agx.at[p, m], xypeer(rel))

    def forward(p, m):
        arrived(s_all.at[p, m, :, pl.ds(0, SENT)], agx.at[p, m])
        term = lax.dot_general(
            w[m].reshape(3 * PAD, CHUNK), s_all[p, m], (((1,), (1,)), ((), ())), preferred_element_type=F32
        )

        @pl.when(m == 0)
        def _():
            acc[...] = term

        @pl.when(m != 0)
        def _():
            acc[...] += term

    def gathered(ref, row, stride):
        lo = ref[pl.ds(row, NZ, stride=stride), :]
        hi = ref[pl.ds(NZ * stride + row, NZ, stride=stride), :]
        return jnp.concatenate([lo, hi], axis=0)

    for i in range(OWN):
        arrived(iall.at[i, pl.ds(0, SRC - 1)], one.at[6 + i])
        wide[...] = iall[i].reshape(SRC * per_side, 128).astype(F32)
        for tl in range(per_side):
            m, pos = divmod(tl, SIDE // 128)
            lanes = at(xh * SIDE + pos * 128, 128)
            s_all[i, m, rows_y, lanes] = gathered(wide, tl, per_side).astype(BF16)
            if pos == SIDE // 128 - 1:
                spread(i, m)

    arrived(dall.at[pl.ds(0, 16 * (SRC - 1)), :], one.at[1])
    for i in range(OWN):
        for tt in range(TILES):
            state[i, :, tt * 128 : (tt + 1) * 128] = gathered(dall, i * TILES + tt, 16)

    @pl.loop(0, PART)
    def _(m):
        for k in range(3):
            for half in range(NX):
                weight_copy(m, k, half).wait()
        forward(0, m)

    def factors(p):
        h = rem(p, OWN)

        def part(q, total):
            r = q * 64
            pa, pb, pc = (acc[at(k * PAD + r, 64), :] for k in range(3))
            e = jnp.exp(-jnp.abs(pa))
            soft = jnp.maximum(pa, 0.0) + jnp.log1p(e)
            inv = 1.0 / (1.0 + e)
            sig = jnp.where(pa >= 0, inv, e * inv)
            tan = jnp.tanh(pb)
            st = soft * tan
            fac[at(r, 64), :] = (sig * tan * pc).astype(BF16)
            fac[at(PAD + r, 64), :] = (soft * (1.0 - tan * tan) * pc).astype(BF16)
            fac[at(2 * PAD + r, 64), :] = st.astype(BF16)
            return total + jnp.sum(st * pc, axis=0, keepdims=True)

        total = lax.fori_loop(0, PAD // 64, part, jnp.zeros((1, ROWS), F32))
        esum[pl.ds(h, 1), 0:ROWS] += total

    def backward(p):
        factors(p)

        @pl.loop(0, PART)
        def _(m):
            g = lax.dot_general(
                fac[...], w[m].reshape(3 * PAD, CHUNK), (((0,), (0,)), ((), ())), preferred_element_type=F32
            )
            g_all[p, m] = g.astype(BF16)
            for rel in FAR_XY:
                to = xypeer(rel)
                block = g_all.at[p, m, at(to[1] * BLOCK, BLOCK), at(to[2] * SIDE, SIDE)]
                push(block, rx.at[p, m, rel - 1], sndg.at[p], rxs.at[p, m], to)

    def plane_sum(p, m):
        arrived(rx.at[p, m], rxs.at[p, m])
        total = g_all[p, m, rows_y, side].astype(F32)
        for k in range(PEERS):
            total = total + rx[p, m, k].astype(F32)
        zs[p, m] = total.astype(BF16)
        for jj in range(PAIR):
            j = m * PAIR + jj

            @pl.when(j == z)
            def _():
                zown[...] = total[:, jj * COLS : (jj + 1) * COLS]

            @pl.when(j != z)
            def _():
                dz = rem(j - z + NZ, NZ)
                push(
                    zs.at[p, m, :, pl.ds(jj * COLS, COLS)], zx.at[p, dz - 1], snd.at[3], zxs.at[p],
                    (j, y, xh, xl, core),
                )

    def update(p, n, h):
        arrived(zx.at[p], zxs.at[p])
        grad = zown[...]
        for k in range(NZ - 1):
            grad = grad + zx[p, k].astype(F32)
        beta = jnp.asarray(n + 1, jnp.int32).astype(F32) / STEPS
        for tt in range(TILES):
            cols = slice(tt * 128, (tt + 1) * 128)
            extra = gathered(dall, ((n + 1) * OWN + h) * TILES + tt, 16)
            old = state[h, :, cols]
            state[h, :, cols] = old - 0.05 * (old + beta * grad[:, cols]) + math.sqrt(0.1) * extra

    own_lanes = at(xh * SIDE + rem(z, PAIR) * COLS, COLS)

    def step_on(p):
        n, h = p // OWN, rem(p, OWN)
        update(p, n, h)

        @pl.when(n < STEPS - 1)
        def _():
            block = s_all.at[p + OWN, z // PAIR, rows_y, own_lanes]
            block[...] = state[h].astype(BF16)
            for dz in FAR_Z:
                push(block, block, snd.at[4], agz.at[p, z], zpeer(dz))

    def pass_on(p, m):
        for jj in range(PAIR):
            j = m * PAIR + jj

            @pl.when(j != z)
            def _():
                arrived(s_all.at[p + OWN, m, rows_y, at(xh * SIDE + jj * COLS, COLS)], agz.at[p, j])

        spread(p + OWN, m)

    early = z < NZ // 2

    def phase(p, carry):
        backward(p)

        @pl.when(p > 0)
        def _():
            @pl.when(jnp.logical_not(early))
            def _():
                step_on(p - 1)

            @pl.loop(0, PART)
            def _(m):
                pass_on(p - 1, m)

        @pl.loop(0, PART)
        def _(m):
            plane_sum(p, m)

        @pl.loop(0, PART)
        def _(m):
            forward(p + 1, m)

        @pl.when(early)
        def _():
            step_on(p)

        return carry

    lax.fori_loop(0, PHASES - 1, phase, 0)

    row = lax.broadcasted_iota(jnp.int32, (8, 128), 0)
    lane = lax.broadcasted_iota(jnp.int32, (8, 128), 1)
    own_lane = y * BLOCK + slot

    last = PHASES - 1
    backward(last)

    inputs[2].wait()
    v = esum[...] / STEPS
    for i in range(OWN):
        v = v - jnp.where((row == i) & (lane == own_lane), slw_ref[i], 0.0)
    e1[...] = v
    for rel in range(1, PEERS + 1):
        push(e1, ex.at[rel - 1], snd.at[5], one.at[3], xypeer(rel))

    @pl.when(jnp.logical_not(early))
    def _():
        update(last - 1, STEPS - 1, 0)

    @pl.loop(0, PART)
    def _(m):
        plane_sum(last, m)

    arrived(ex, one.at[3])
    total = e1[...]
    for k in range(PEERS):
        total = total + ex[k]
    e2[...] = total
    for dz in range(1, NZ):
        push(e2, ez.at[dz - 1], snd.at[6], one.at[4], zpeer(dz))

    update(last, STEPS - 1, 1)
    for i in range(OWN):
        for tt in range(TILES):
            tile = state[i, :, tt * 128 : (tt + 1) * 128]
            fsend[pl.ds(i * TILES + tt, NZ, stride=8), :] = tile[0:NZ]
            fsend[pl.ds(NZ * 8 + i * TILES + tt, NZ, stride=8), :] = tile[NZ:]
    for k in FAR_ZX:
        to = zxpeer(k)
        push(fsend.at[at((to[2] * NZ + to[0]) * 8, 8), :], fall.at[slot], snd.at[8], one.at[2], to)
    fall[slot] = fsend[at(slot * 8, 8), :]

    arrived(ez, one.at[4])
    total = e2[...]
    for k in range(NZ - 1):
        total = total + ez[k]
    e3[...] = -total
    for k in range(1, 4):
        push(e3, el.at[k - 1], snd.at[7], one.at[5], gpeer(k))
    for i in range(OWN):
        lw_ref[i] = jnp.sum(jnp.where((row == i) & (lane == own_lane), -total, 0.0))
    arrived(el, one.at[5])
    used = (row < OWN) & (lane < ROWS)
    lws = [jnp.where(used, v, -jnp.inf) for v in [-total] + [el[k] for k in range(3)]]
    top = jnp.max(jnp.maximum(jnp.maximum(lws[0], lws[1]), jnp.maximum(lws[2], lws[3])))
    mass = jnp.sum(sum(jnp.exp(v - top) for v in lws))
    lr_ref[0] = jnp.max(top + jnp.log(jnp.full((8, 128), mass, F32)) - math.log(4 * OWN * ROWS))

    arrived(fall.at[pl.ds(0, SRC - 1)], one.at[2])
    for src in range(SRC):
        for i in range(OWN):
            for tt in range(TILES):
                c = (src * TILES + tt) * 128
                out_ref[i : i + 1, c : c + 128] = fall[src, i * TILES + tt : i * TILES + tt + 1, :]

    left(iall.at[:, pl.ds(0, SRC - 1)], snd.at[0])
    left(dpack.at[pl.ds(0, SRC - 1)], snd.at[1])
    left(s_all.at[:, :, :, pl.ds(0, SENT)], snd.at[2])
    left(zx, snd.at[3])
    left(zx.at[pl.ds(0, PHASES - OWN)], snd.at[4])
    left(ex, snd.at[5])
    left(ez, snd.at[6])
    left(el, snd.at[7])
    left(fall.at[pl.ds(0, SRC - 1)], snd.at[8])
    for p in range(PHASES):
        left(g_all.at[p, :, :, pl.ds(0, SENT)], sndg.at[p])


def per_device(start_state, start_log_weight, noise, first_weight, second_weight, third_weight):
    smem = pl.BlockSpec(memory_space=pltpu.SMEM)
    hbm = pl.BlockSpec(memory_space=pl.ANY)
    tile = (8, 128)
    state, log_weight, log_ratio = pl.pallas_call(
        kernel,
        out_shape=(
            jax.ShapeDtypeStruct((OWN, D), F32),
            jax.ShapeDtypeStruct((OWN,), F32),
            jax.ShapeDtypeStruct((1,), F32),
        ),
        in_specs=[hbm] * 6,
        out_specs=(pl.BlockSpec(memory_space=pltpu.VMEM), smem, smem),
        scratch_shapes=[
            pltpu.VMEM((OWN, D), F32),
            pltpu.SMEM((OWN,), F32),
            pltpu.VMEM((STEPS, OWN, D), BF16),
            pltpu.VMEM((PART, 3, PAD, CHUNK), BF16),
            pltpu.VMEM((PHASES, PART, ROWS, CHUNK), BF16),
            pltpu.VMEM((PHASES, PART, ROWS, CHUNK), BF16),
            pltpu.VMEM((PHASES, PART, PEERS, BLOCK, SIDE), BF16),
            pltpu.VMEM((PHASES, PART, BLOCK, SIDE), BF16),
            pltpu.VMEM((PHASES, NZ - 1, BLOCK, COLS), BF16),
            pltpu.VMEM((BLOCK, COLS), F32),
            pltpu.VMEM((OWN, BLOCK, COLS), F32),
            pltpu.VMEM((3 * PAD, ROWS), F32),
            pltpu.VMEM((3 * PAD, ROWS), BF16),
            pltpu.VMEM(tile, F32),
            pltpu.VMEM((NX, OWN, 16, 128), F32),
            pltpu.VMEM((OWN, SRC, 16, 128), BF16),
            pltpu.VMEM((OWN, NX, 16, 128), BF16),
            pltpu.VMEM((SRC * 16, 128), F32),
            pltpu.VMEM((SRC, 16, 128), F32),
            pltpu.VMEM((SRC * 16, 128), F32),
            pltpu.VMEM((SRC * 8, 128), F32),
            pltpu.VMEM((SRC, 8, 128), F32),
            pltpu.VMEM(tile, F32),
            pltpu.VMEM((PEERS, *tile), F32),
            pltpu.VMEM(tile, F32),
            pltpu.VMEM((NZ - 1, *tile), F32),
            pltpu.VMEM(tile, F32),
            pltpu.VMEM((3, *tile), F32),
            pltpu.SemaphoreType.DMA((3,)),
            pltpu.SemaphoreType.DMA((PART, 3, NX)),
            pltpu.SemaphoreType.DMA((PHASES, PART)),
            pltpu.SemaphoreType.DMA((PHASES - OWN, NZ)),
            pltpu.SemaphoreType.DMA((PHASES, PART)),
            pltpu.SemaphoreType.DMA((PHASES,)),
            pltpu.SemaphoreType.DMA((8,)),
            pltpu.SemaphoreType.DMA((9,)),
            pltpu.SemaphoreType.DMA((PHASES,)),
        ],
        compiler_params=pltpu.CompilerParams(
            collective_id=0, has_side_effects=True, vmem_limit_bytes=67043328
        ),
    )(start_state, start_log_weight, noise, first_weight, second_weight, third_weight)
    return state, log_weight, log_ratio[0]


def solution(mesh):
    torus = Mesh(mesh.devices.reshape(8, 4, 2, 2, 2), AXES)
    placed = (
        P(BLK_GRP, None),
        P(BLK_GRP),
        P(None, BLK_GRP, None),
        P(BLK, None),
        P(BLK, None),
        P(BLK, None),
    )
    return jax.shard_map(
        per_device,
        mesh=torus,
        in_specs=placed,
        out_specs=(P(BLK_GRP, None), P(BLK_GRP), P()),
        check_vma=False,
    )
```

```python
import math

import jax
import jax.numpy as jnp
from jax import lax
from jax.experimental import pallas as pl
from jax.experimental.pallas import tpu as pltpu
from jax.sharding import Mesh
from jax.sharding import PartitionSpec as P

BLK = ("blk_0", "blk_1", "blk_2")
BLK_GRP = ("blk_0", "blk_1", "blk_2", "grp_0", "grp_1")
AXES = BLK_GRP
MESH = pl.DeviceIdType.MESH
F32 = jnp.float32
BF16 = jnp.bfloat16

NZ, NY, NX = 8, 4, 2
OWN = 2
BLOCK = NX * NZ
ROWS = NY * BLOCK
STEPS = 3
PHASES = STEPS * OWN
D = 4096
COLS = D // (NX * NZ)
PART = 4
SIDE = D // (NX * PART)
CHUNK = NX * SIDE
PAIR = SIDE // COLS
TILES = COLS // 128
SRC = NX * NZ
PAD = 256
PEERS = NY * NX - 1
SENT = CHUNK * PEERS // (PEERS + 1)
FAR_XY = (5, 4, 3, 7, 2, 6, 1)
FAR_Z = (4, 3, 5, 2, 6, 1, 7)
FAR_ZX = tuple(NX * dz + 1 for dz in FAR_Z[:3]) + tuple(NX * dz for dz in FAR_Z[:3]) + tuple(
    NX * dz + dx for dz in FAR_Z[3:] for dx in (1, 0)
) + (1,)


def rem(a, n):
    return lax.rem(a, n)


def at(start, size):
    return pl.ds(pl.multiple_of(start, size), size)


def kernel(
    start_hbm, slw_hbm, noise_hbm, w1_ref, w2_ref, w3_ref,
    out_ref, lw_ref, lr_ref,
    start_ref, slw_ref, noise_ref,
    w, s_all, g_all, rx, zs, zx, zown, state, acc, fac, esum,
    ipack, iall, conv, wide, dpack, dall, fsend, fall, e1, ex, e2, ez, e3, el,
    insem, wsem, agx, agz, rxs, zxs, one, snd, sndg,
):
    z, y, xh, xl, core = (lax.axis_index(name) for name in AXES)
    width = w1_ref.shape[0]
    rows_y = at(y * BLOCK, BLOCK)
    side = at(xh * SIDE, SIDE)
    slot = xh * NZ + z

    def zpeer(dz):
        return (rem(z + dz, NZ), y, xh, xl, core)

    def xypeer(rel):
        dy, dx = divmod(rel, NX)
        return (z, rem(y + dy, NY), rem(xh + dx, NX), rem(xl + dx, NX), core)

    def zxpeer(k):
        dz, dx = divmod(k, NX)
        return (rem(z + dz, NZ), y, rem(xh + dx, NX), rem(xl + dx, NX), core)

    def gpeer(k):
        dl, dc = divmod(k, 2)
        return (z, y, xh, rem(xl + dl, 2), rem(core + dc, 2))

    def push(src, dst, send, recv, to):
        pltpu.make_async_remote_copy(
            src_ref=src, dst_ref=dst, send_sem=send, recv_sem=recv, device_id=to, device_id_type=MESH
        ).start()

    def arrived(ref, recv):
        pltpu.make_async_remote_copy(
            src_ref=ref, dst_ref=ref, send_sem=snd.at[0], recv_sem=recv,
            device_id=zpeer(1), device_id_type=MESH,
        ).wait_recv()

    def left(ref, send):
        pltpu.make_async_remote_copy(
            src_ref=ref, dst_ref=ref, send_sem=send, recv_sem=one.at[0],
            device_id=zpeer(1), device_id_type=MESH,
        ).wait_send()

    inputs = (
        pltpu.make_async_copy(start_hbm, start_ref, insem.at[0]),
        pltpu.make_async_copy(noise_hbm, noise_ref, insem.at[1]),
        pltpu.make_async_copy(slw_hbm, slw_ref, insem.at[2]),
    )
    for copy in inputs:
        copy.start()

    barrier = pltpu.get_barrier_semaphore()
    greeted = (
        [zxpeer(k) for k in range(1, SRC)]
        + [xypeer(r) for r in range(2, PEERS + 1)]
        + [gpeer(k) for k in range(1, 4)]
    )
    for to in greeted:
        pl.semaphore_signal(barrier, inc=1, device_id=to, device_id_type=MESH)

    weights = (w1_ref, w2_ref, w3_ref)

    def weight_copy(m, k, half):
        return pltpu.make_async_copy(
            weights[k].at[:, at(half * (D // NX) + m * SIDE, SIDE)],
            w.at[m, k, pl.ds(0, width), pl.ds(half * SIDE, SIDE)],
            wsem.at[m, k, half],
        )

    @pl.loop(0, PART)
    def _(m):
        for k in range(3):
            for half in range(NX):
                weight_copy(m, k, half).start()

    per_side = D // NX // 128
    inputs[0].wait()
    for t in range(D // 128):
        v = start_ref[:, t * 128 : (t + 1) * 128]
        xs, tl = divmod(t, per_side)
        for i in range(OWN):
            ipack[xs, i, tl : tl + 1, :] = v[i : i + 1]
            r = i * TILES + tl % TILES
            dpack[xs * NZ + tl // TILES, r : r + 1, :] = v[i : i + 1]
    for i in range(OWN):
        conv[i] = ipack[:, i].astype(BF16)
        iall[i, slot] = conv[i, xh]

    pl.semaphore_wait(barrier, len(greeted))

    for i in range(OWN):
        for k in FAR_ZX:
            to = zxpeer(k)
            push(conv.at[i, to[2]], iall.at[i, slot], snd.at[0], one.at[6 + i], to)

    inputs[1].wait()
    for k in range(STEPS):
        for t in range(D // 128):
            v = noise_ref[k, :, t * 128 : (t + 1) * 128].astype(F32)
            xs, tl = divmod(t, per_side)
            for i in range(OWN):
                r = (k + 1) * OWN * TILES + i * TILES + tl % TILES
                dpack[xs * NZ + tl // TILES, r : r + 1, :] = v[i : i + 1]
    dall[at(slot * 16, 16), :] = dpack[slot]
    for k in FAR_ZX:
        to = zxpeer(k)
        push(dpack.at[to[2] * NZ + to[0]], dall.at[at(slot * 16, 16), :], snd.at[1], one.at[1], to)

    @pl.loop(0, PART)
    def _(m):
        for k in range(3):
            w[m, k, width:PAD, :] = jnp.zeros((PAD - width, CHUNK), BF16)

    esum[...] = jnp.zeros_like(esum)
    fsend[...] = jnp.zeros_like(fsend)

    def spread(p, m):
        for rel in FAR_XY:
            block = s_all.at[p, m, rows_y, side]
            push(block, block, snd.at[2], agx.at[p, m], xypeer(rel))

    def forward(p, m):
        arrived(s_all.at[p, m, :, pl.ds(0, SENT)], agx.at[p, m])
        term = lax.dot_general(
            w[m].reshape(3 * PAD, CHUNK), s_all[p, m], (((1,), (1,)), ((), ())), preferred_element_type=F32
        )

        @pl.when(m == 0)
        def _():
            acc[...] = term

        @pl.when(m != 0)
        def _():
            acc[...] += term

    def gathered(ref, row, stride):
        lo = ref[pl.ds(row, NZ, stride=stride), :]
        hi = ref[pl.ds(NZ * stride + row, NZ, stride=stride), :]
        return jnp.concatenate([lo, hi], axis=0)

    for i in range(OWN):
        arrived(iall.at[i, pl.ds(0, SRC - 1)], one.at[6 + i])
        wide[...] = iall[i].reshape(SRC * per_side, 128).astype(F32)
        for tl in range(per_side):
            m, pos = divmod(tl, SIDE // 128)
            lanes = at(xh * SIDE + pos * 128, 128)
            s_all[i, m, rows_y, lanes] = gathered(wide, tl, per_side).astype(BF16)
            if pos == SIDE // 128 - 1:
                spread(i, m)

    arrived(dall.at[pl.ds(0, 16 * (SRC - 1)), :], one.at[1])
    for i in range(OWN):
        for tt in range(TILES):
            state[i, :, tt * 128 : (tt + 1) * 128] = gathered(dall, i * TILES + tt, 16)

    @pl.loop(0, PART)
    def _(m):
        for k in range(3):
            for half in range(NX):
                weight_copy(m, k, half).wait()
        forward(0, m)

    def factors(p):
        h = rem(p, OWN)

        def part(q, total):
            r = q * 64
            pa, pb, pc = (acc[at(k * PAD + r, 64), :] for k in range(3))
            e = jnp.exp(-jnp.abs(pa))
            soft = jnp.maximum(pa, 0.0) + jnp.log1p(e)
            inv = 1.0 / (1.0 + e)
            sig = jnp.where(pa >= 0, inv, e * inv)
            tan = jnp.tanh(pb)
            st = soft * tan
            fac[at(r, 64), :] = (sig * tan * pc).astype(BF16)
            fac[at(PAD + r, 64), :] = (soft * (1.0 - tan * tan) * pc).astype(BF16)
            fac[at(2 * PAD + r, 64), :] = st.astype(BF16)
            return total + jnp.sum(st * pc, axis=0, keepdims=True)

        total = lax.fori_loop(0, PAD // 64, part, jnp.zeros((1, ROWS), F32))
        esum[pl.ds(h, 1), 0:ROWS] += total

    def backward(p):
        factors(p)

        @pl.loop(0, PART)
        def _(m):
            g = lax.dot_general(
                fac[...], w[m].reshape(3 * PAD, CHUNK), (((0,), (0,)), ((), ())), preferred_element_type=F32
            )
            g_all[p, m] = g.astype(BF16)
            for rel in FAR_XY:
                to = xypeer(rel)
                block = g_all.at[p, m, at(to[1] * BLOCK, BLOCK), at(to[2] * SIDE, SIDE)]
                push(block, rx.at[p, m, rel - 1], sndg.at[p], rxs.at[p, m], to)

    def plane_sum(p, m):
        arrived(rx.at[p, m], rxs.at[p, m])
        total = g_all[p, m, rows_y, side].astype(F32)
        for k in range(PEERS):
            total = total + rx[p, m, k].astype(F32)
        zs[p, m] = total.astype(BF16)
        for jj in range(PAIR):
            j = m * PAIR + jj

            @pl.when(j == z)
            def _():
                zown[rem(p, OWN)] = total[:, jj * COLS : (jj + 1) * COLS]

            @pl.when(j != z)
            def _():
                dz = rem(j - z + NZ, NZ)
                push(
                    zs.at[p, m, :, pl.ds(jj * COLS, COLS)], zx.at[p, dz - 1], snd.at[3], zxs.at[p],
                    (j, y, xh, xl, core),
                )

    def update(p, n, h):
        arrived(zx.at[p], zxs.at[p])
        grad = zown[h]
        for k in range(NZ - 1):
            grad = grad + zx[p, k].astype(F32)
        beta = jnp.asarray(n + 1, jnp.int32).astype(F32) / STEPS
        for tt in range(TILES):
            cols = slice(tt * 128, (tt + 1) * 128)
            extra = gathered(dall, ((n + 1) * OWN + h) * TILES + tt, 16)
            old = state[h, :, cols]
            state[h, :, cols] = old - 0.05 * (old + beta * grad[:, cols]) + math.sqrt(0.1) * extra

    own_lanes = at(xh * SIDE + rem(z, PAIR) * COLS, COLS)

    def step_on(p):
        n, h = p // OWN, rem(p, OWN)
        update(p, n, h)

        block = s_all.at[p + OWN, z // PAIR, rows_y, own_lanes]
        block[...] = state[h].astype(BF16)
        for dz in FAR_Z:
            push(block, block, snd.at[4], agz.at[p, z], zpeer(dz))

    def pass_on(p, m):
        for jj in range(PAIR):
            j = m * PAIR + jj

            @pl.when(j != z)
            def _():
                arrived(s_all.at[p + OWN, m, rows_y, at(xh * SIDE + jj * COLS, COLS)], agz.at[p, j])

        spread(p + OWN, m)

    def each(part, *args):
        @pl.loop(0, PART)
        def _(m):
            part(*args, m)

    def step(n, carry):
        first, second = n * OWN, n * OWN + 1
        backward(first)
        each(forward, second)
        backward(second)
        each(plane_sum, first)
        each(plane_sum, second)
        step_on(first)
        step_on(second)
        each(pass_on, first)
        each(pass_on, second)
        each(forward, first + OWN)
        return carry

    lax.fori_loop(0, STEPS - 1, step, 0)

    row = lax.broadcasted_iota(jnp.int32, (8, 128), 0)
    lane = lax.broadcasted_iota(jnp.int32, (8, 128), 1)
    own_lane = y * BLOCK + slot

    last = PHASES - 1
    backward(last - 1)
    each(forward, last)
    backward(last)

    inputs[2].wait()
    v = esum[...] / STEPS
    for i in range(OWN):
        v = v - jnp.where((row == i) & (lane == own_lane), slw_ref[i], 0.0)
    e1[...] = v
    for rel in range(1, PEERS + 1):
        push(e1, ex.at[rel - 1], snd.at[5], one.at[3], xypeer(rel))

    each(plane_sum, last - 1)
    arrived(ex, one.at[3])
    total = e1[...]
    for k in range(PEERS):
        total = total + ex[k]
    e2[...] = total
    for dz in range(1, NZ):
        push(e2, ez.at[dz - 1], snd.at[6], one.at[4], zpeer(dz))

    each(plane_sum, last)
    update(last - 1, STEPS - 1, 0)
    update(last, STEPS - 1, 1)
    for i in range(OWN):
        for tt in range(TILES):
            tile = state[i, :, tt * 128 : (tt + 1) * 128]
            fsend[pl.ds(i * TILES + tt, NZ, stride=8), :] = tile[0:NZ]
            fsend[pl.ds(NZ * 8 + i * TILES + tt, NZ, stride=8), :] = tile[NZ:]
    for k in FAR_ZX:
        to = zxpeer(k)
        push(fsend.at[at((to[2] * NZ + to[0]) * 8, 8), :], fall.at[slot], snd.at[8], one.at[2], to)
    fall[slot] = fsend[at(slot * 8, 8), :]

    arrived(ez, one.at[4])
    total = e2[...]
    for k in range(NZ - 1):
        total = total + ez[k]
    e3[...] = -total
    for k in range(1, 4):
        push(e3, el.at[k - 1], snd.at[7], one.at[5], gpeer(k))
    for i in range(OWN):
        lw_ref[i] = jnp.sum(jnp.where((row == i) & (lane == own_lane), -total, 0.0))
    arrived(el, one.at[5])
    used = (row < OWN) & (lane < ROWS)
    lws = [jnp.where(used, v, -jnp.inf) for v in [-total] + [el[k] for k in range(3)]]
    top = jnp.max(jnp.maximum(jnp.maximum(lws[0], lws[1]), jnp.maximum(lws[2], lws[3])))
    mass = jnp.sum(sum(jnp.exp(v - top) for v in lws))
    lr_ref[0] = jnp.max(top + jnp.log(jnp.full((8, 128), mass, F32)) - math.log(4 * OWN * ROWS))

    arrived(fall.at[pl.ds(0, SRC - 1)], one.at[2])
    for src in range(SRC):
        for i in range(OWN):
            for tt in range(TILES):
                c = (src * TILES + tt) * 128
                out_ref[i : i + 1, c : c + 128] = fall[src, i * TILES + tt : i * TILES + tt + 1, :]

    left(iall.at[:, pl.ds(0, SRC - 1)], snd.at[0])
    left(dpack.at[pl.ds(0, SRC - 1)], snd.at[1])
    left(s_all.at[:, :, :, pl.ds(0, SENT)], snd.at[2])
    left(zx, snd.at[3])
    left(zx.at[pl.ds(0, PHASES - OWN)], snd.at[4])
    left(ex, snd.at[5])
    left(ez, snd.at[6])
    left(el, snd.at[7])
    left(fall.at[pl.ds(0, SRC - 1)], snd.at[8])
    for p in range(PHASES):
        left(g_all.at[p, :, :, pl.ds(0, SENT)], sndg.at[p])


def per_device(start_state, start_log_weight, noise, first_weight, second_weight, third_weight):
    smem = pl.BlockSpec(memory_space=pltpu.SMEM)
    hbm = pl.BlockSpec(memory_space=pl.ANY)
    tile = (8, 128)
    state, log_weight, log_ratio = pl.pallas_call(
        kernel,
        out_shape=(
            jax.ShapeDtypeStruct((OWN, D), F32),
            jax.ShapeDtypeStruct((OWN,), F32),
            jax.ShapeDtypeStruct((1,), F32),
        ),
        in_specs=[hbm] * 6,
        out_specs=(pl.BlockSpec(memory_space=pltpu.VMEM), smem, smem),
        scratch_shapes=[
            pltpu.VMEM((OWN, D), F32),
            pltpu.SMEM((OWN,), F32),
            pltpu.VMEM((STEPS, OWN, D), BF16),
            pltpu.VMEM((PART, 3, PAD, CHUNK), BF16),
            pltpu.VMEM((PHASES, PART, ROWS, CHUNK), BF16),
            pltpu.VMEM((PHASES, PART, ROWS, CHUNK), BF16),
            pltpu.VMEM((PHASES, PART, PEERS, BLOCK, SIDE), BF16),
            pltpu.VMEM((PHASES, PART, BLOCK, SIDE), BF16),
            pltpu.VMEM((PHASES, NZ - 1, BLOCK, COLS), BF16),
            pltpu.VMEM((OWN, BLOCK, COLS), F32),
            pltpu.VMEM((OWN, BLOCK, COLS), F32),
            pltpu.VMEM((3 * PAD, ROWS), F32),
            pltpu.VMEM((3 * PAD, ROWS), BF16),
            pltpu.VMEM(tile, F32),
            pltpu.VMEM((NX, OWN, 16, 128), F32),
            pltpu.VMEM((OWN, SRC, 16, 128), BF16),
            pltpu.VMEM((OWN, NX, 16, 128), BF16),
            pltpu.VMEM((SRC * 16, 128), F32),
            pltpu.VMEM((SRC, 16, 128), F32),
            pltpu.VMEM((SRC * 16, 128), F32),
            pltpu.VMEM((SRC * 8, 128), F32),
            pltpu.VMEM((SRC, 8, 128), F32),
            pltpu.VMEM(tile, F32),
            pltpu.VMEM((PEERS, *tile), F32),
            pltpu.VMEM(tile, F32),
            pltpu.VMEM((NZ - 1, *tile), F32),
            pltpu.VMEM(tile, F32),
            pltpu.VMEM((3, *tile), F32),
            pltpu.SemaphoreType.DMA((3,)),
            pltpu.SemaphoreType.DMA((PART, 3, NX)),
            pltpu.SemaphoreType.DMA((PHASES, PART)),
            pltpu.SemaphoreType.DMA((PHASES - OWN, NZ)),
            pltpu.SemaphoreType.DMA((PHASES, PART)),
            pltpu.SemaphoreType.DMA((PHASES,)),
            pltpu.SemaphoreType.DMA((8,)),
            pltpu.SemaphoreType.DMA((9,)),
            pltpu.SemaphoreType.DMA((PHASES,)),
        ],
        compiler_params=pltpu.CompilerParams(
            collective_id=0, has_side_effects=True, vmem_limit_bytes=67043328
        ),
    )(start_state, start_log_weight, noise, first_weight, second_weight, third_weight)
    return state, log_weight, log_ratio[0]


def solution(mesh):
    torus = Mesh(mesh.devices.reshape(8, 4, 2, 2, 2), AXES)
    placed = (
        P(BLK_GRP, None),
        P(BLK_GRP),
        P(None, BLK_GRP, None),
        P(BLK, None),
        P(BLK, None),
        P(BLK, None),
    )
    return jax.shard_map(
        per_device,
        mesh=torus,
        in_specs=placed,
        out_specs=(P(BLK_GRP, None), P(BLK_GRP), P()),
        check_vma=False,
    )
```

```python
import math

import jax
import jax.numpy as jnp
from jax import lax
from jax.experimental import pallas as pl
from jax.experimental.pallas import tpu as pltpu
from jax.sharding import Mesh
from jax.sharding import PartitionSpec as P

BLK = ("blk_0", "blk_1", "blk_2")
BLK_GRP = ("blk_0", "blk_1", "blk_2", "grp_0", "grp_1")
AXES = BLK_GRP
MESH = pl.DeviceIdType.MESH
F32 = jnp.float32
BF16 = jnp.bfloat16

NZ, NY, NX = 8, 4, 2
OWN = 2
BLOCK = NX * NZ
ROWS = NY * BLOCK
STEPS = 3
PHASES = STEPS * OWN
D = 4096
COLS = D // (NX * NZ)
PART = 4
SIDE = D // (NX * PART)
CHUNK = NX * SIDE
PAIR = SIDE // COLS
TILES = COLS // 128
SRC = NX * NZ
PAD = 256
PEERS = NY * NX - 1
SENT = CHUNK * PEERS // (PEERS + 1)
FAR_XY = (5, 4, 3, 7, 2, 6, 1)
FAR_Z = (4, 3, 5, 2, 6, 1, 7)
FAR_ZX = tuple(NX * dz + 1 for dz in FAR_Z[:3]) + tuple(NX * dz for dz in FAR_Z[:3]) + tuple(
    NX * dz + dx for dz in FAR_Z[3:] for dx in (1, 0)
) + (1,)


def rem(a, n):
    return lax.rem(a, n)


def at(start, size):
    return pl.ds(pl.multiple_of(start, size), size)


def kernel(
    start_hbm, slw_hbm, noise_hbm, w1_ref, w2_ref, w3_ref,
    out_ref, lw_ref, lr_ref,
    start_ref, slw_ref, noise_ref,
    w, s_all, g_all, rx, zs, zx, zown, state, acc, fac, esum,
    ipack, iall, conv, wide, dpack, dall, fsend, fall, e1, ex, e2, ez, e3, el,
    insem, wsem, agx, agz, rxs, zxs, one, snd, sndg,
):
    z, y, xh, xl, core = (lax.axis_index(name) for name in AXES)
    width = w1_ref.shape[0]
    rows_y = at(y * BLOCK, BLOCK)
    side = at(xh * SIDE, SIDE)
    slot = xh * NZ + z

    def zpeer(dz):
        return (rem(z + dz, NZ), y, xh, xl, core)

    def xypeer(rel):
        dy, dx = divmod(rel, NX)
        return (z, rem(y + dy, NY), rem(xh + dx, NX), rem(xl + dx, NX), core)

    def zxpeer(k):
        dz, dx = divmod(k, NX)
        return (rem(z + dz, NZ), y, rem(xh + dx, NX), rem(xl + dx, NX), core)

    def gpeer(k):
        dl, dc = divmod(k, 2)
        return (z, y, xh, rem(xl + dl, 2), rem(core + dc, 2))

    def push(src, dst, send, recv, to):
        pltpu.make_async_remote_copy(
            src_ref=src, dst_ref=dst, send_sem=send, recv_sem=recv, device_id=to, device_id_type=MESH
        ).start()

    def arrived(ref, recv):
        pltpu.make_async_remote_copy(
            src_ref=ref, dst_ref=ref, send_sem=snd.at[0], recv_sem=recv,
            device_id=zpeer(1), device_id_type=MESH,
        ).wait_recv()

    def left(ref, send):
        pltpu.make_async_remote_copy(
            src_ref=ref, dst_ref=ref, send_sem=send, recv_sem=one.at[0],
            device_id=zpeer(1), device_id_type=MESH,
        ).wait_send()

    inputs = (
        pltpu.make_async_copy(start_hbm, start_ref, insem.at[0]),
        pltpu.make_async_copy(noise_hbm, noise_ref, insem.at[1]),
        pltpu.make_async_copy(slw_hbm, slw_ref, insem.at[2]),
    )
    for copy in inputs:
        copy.start()

    barrier = pltpu.get_barrier_semaphore()
    greeted = (
        [zxpeer(k) for k in range(1, SRC)]
        + [xypeer(r) for r in range(2, PEERS + 1)]
        + [gpeer(k) for k in range(1, 4)]
    )
    for to in greeted:
        pl.semaphore_signal(barrier, inc=1, device_id=to, device_id_type=MESH)

    weights = (w1_ref, w2_ref, w3_ref)

    def weight_copy(m, k, half):
        return pltpu.make_async_copy(
            weights[k].at[:, at(half * (D // NX) + m * SIDE, SIDE)],
            w.at[m, k, pl.ds(0, width), pl.ds(half * SIDE, SIDE)],
            wsem.at[m, k, half],
        )

    @pl.loop(0, PART)
    def _(m):
        for k in range(3):
            for half in range(NX):
                weight_copy(m, k, half).start()

    per_side = D // NX // 128
    inputs[0].wait()
    for t in range(D // 128):
        v = start_ref[:, t * 128 : (t + 1) * 128]
        xs, tl = divmod(t, per_side)
        for i in range(OWN):
            ipack[xs, i, tl : tl + 1, :] = v[i : i + 1]
            r = i * TILES + tl % TILES
            dpack[xs * NZ + tl // TILES, r : r + 1, :] = v[i : i + 1]
    for i in range(OWN):
        conv[i] = ipack[:, i].astype(BF16)
        iall[i, slot] = conv[i, xh]

    pl.semaphore_wait(barrier, len(greeted))

    for i in range(OWN):
        for k in FAR_ZX:
            to = zxpeer(k)
            push(conv.at[i, to[2]], iall.at[i, slot], snd.at[0], one.at[6 + i], to)

    inputs[1].wait()
    for k in range(STEPS):
        for t in range(D // 128):
            v = noise_ref[k, :, t * 128 : (t + 1) * 128].astype(F32)
            xs, tl = divmod(t, per_side)
            for i in range(OWN):
                r = (k + 1) * OWN * TILES + i * TILES + tl % TILES
                dpack[xs * NZ + tl // TILES, r : r + 1, :] = v[i : i + 1]
    dall[at(slot * 16, 16), :] = dpack[slot]
    for k in FAR_ZX:
        to = zxpeer(k)
        push(dpack.at[to[2] * NZ + to[0]], dall.at[at(slot * 16, 16), :], snd.at[1], one.at[1], to)

    @pl.loop(0, PART)
    def _(m):
        for k in range(3):
            w[m, k, width:PAD, :] = jnp.zeros((PAD - width, CHUNK), BF16)

    esum[...] = jnp.zeros_like(esum)
    fsend[...] = jnp.zeros_like(fsend)

    def spread(p, m):
        for rel in FAR_XY:
            block = s_all.at[p, m, rows_y, side]
            push(block, block, snd.at[2], agx.at[p, m], xypeer(rel))

    def forward(p, m, start):
        arrived(s_all.at[p, m, :, pl.ds(0, SENT)], agx.at[p, m])
        term = lax.dot_general(
            w[m].reshape(3 * PAD, CHUNK), s_all[p, m], (((1,), (1,)), ((), ())), preferred_element_type=F32
        )

        @pl.when(start)
        def _():
            acc[...] = term

        @pl.when(jnp.logical_not(start))
        def _():
            acc[...] += term

    def gathered(ref, row, stride):
        lo = ref[pl.ds(row, NZ, stride=stride), :]
        hi = ref[pl.ds(NZ * stride + row, NZ, stride=stride), :]
        return jnp.concatenate([lo, hi], axis=0)

    for i in range(OWN):
        arrived(iall.at[i, pl.ds(0, SRC - 1)], one.at[6 + i])
        wide[...] = iall[i].reshape(SRC * per_side, 128).astype(F32)
        for tl in range(per_side):
            m, pos = divmod(tl, SIDE // 128)
            lanes = at(xh * SIDE + pos * 128, 128)
            s_all[i, m, rows_y, lanes] = gathered(wide, tl, per_side).astype(BF16)
            if pos == SIDE // 128 - 1:
                spread(i, m)

    arrived(dall.at[pl.ds(0, 16 * (SRC - 1)), :], one.at[1])
    for i in range(OWN):
        for tt in range(TILES):
            state[i, :, tt * 128 : (tt + 1) * 128] = gathered(dall, i * TILES + tt, 16)

    @pl.loop(0, PART)
    def _(m):
        for k in range(3):
            for half in range(NX):
                weight_copy(m, k, half).wait()
        forward(0, m, m == 0)

    def factors(p):
        h = rem(p, OWN)

        def part(q, total):
            r = q * 64
            pa, pb, pc = (acc[at(k * PAD + r, 64), :] for k in range(3))
            e = jnp.exp(-jnp.abs(pa))
            soft = jnp.maximum(pa, 0.0) + jnp.log1p(e)
            inv = 1.0 / (1.0 + e)
            sig = jnp.where(pa >= 0, inv, e * inv)
            tan = jnp.tanh(pb)
            st = soft * tan
            fac[at(r, 64), :] = (sig * tan * pc).astype(BF16)
            fac[at(PAD + r, 64), :] = (soft * (1.0 - tan * tan) * pc).astype(BF16)
            fac[at(2 * PAD + r, 64), :] = st.astype(BF16)
            return total + jnp.sum(st * pc, axis=0, keepdims=True)

        total = lax.fori_loop(0, PAD // 64, part, jnp.zeros((1, ROWS), F32))
        esum[pl.ds(h, 1), 0:ROWS] += total

    def backward(p):
        factors(p)

        @pl.loop(0, PART)
        def _(m):
            g = lax.dot_general(
                fac[...], w[m].reshape(3 * PAD, CHUNK), (((0,), (0,)), ((), ())), preferred_element_type=F32
            )
            g_all[p, m] = g.astype(BF16)
            for rel in FAR_XY:
                to = xypeer(rel)
                block = g_all.at[p, m, at(to[1] * BLOCK, BLOCK), at(to[2] * SIDE, SIDE)]
                push(block, rx.at[p, m, rel - 1], sndg.at[p], rxs.at[p, m], to)

    def plane_sum(p, m):
        arrived(rx.at[p, m], rxs.at[p, m])
        total = g_all[p, m, rows_y, side].astype(F32)
        for k in range(PEERS):
            total = total + rx[p, m, k].astype(F32)
        zs[p, m] = total.astype(BF16)
        for jj in range(PAIR):
            j = m * PAIR + jj

            @pl.when(j == z)
            def _():
                zown[rem(p, OWN)] = total[:, jj * COLS : (jj + 1) * COLS]

            @pl.when(j != z)
            def _():
                dz = rem(j - z + NZ, NZ)
                push(
                    zs.at[p, m, :, pl.ds(jj * COLS, COLS)], zx.at[p, dz - 1], snd.at[3], zxs.at[p],
                    (j, y, xh, xl, core),
                )

    def update(p, n, h):
        arrived(zx.at[p], zxs.at[p])
        grad = zown[h]
        for k in range(NZ - 1):
            grad = grad + zx[p, k].astype(F32)
        beta = jnp.asarray(n + 1, jnp.int32).astype(F32) / STEPS
        for tt in range(TILES):
            cols = slice(tt * 128, (tt + 1) * 128)
            extra = gathered(dall, ((n + 1) * OWN + h) * TILES + tt, 16)
            old = state[h, :, cols]
            state[h, :, cols] = old - 0.05 * (old + beta * grad[:, cols]) + math.sqrt(0.1) * extra

    def owned(p, j):
        return s_all.at[p, j // PAIR, rows_y, at(xh * SIDE + rem(j, PAIR) * COLS, COLS)]

    def spread_owned(p, j):
        for rel in FAR_XY:
            push(owned(p, j), owned(p, j), snd.at[2], agx.at[p, j // PAIR], xypeer(rel))

    def step_on(p):
        n, h = p // OWN, rem(p, OWN)
        update(p, n, h)

        block = owned(p + OWN, z)
        block[...] = state[h].astype(BF16)
        for dz in FAR_Z:
            push(block, block, snd.at[4], agz.at[p, z], zpeer(dz))
        spread_owned(p + OWN, z)

    def pass_on(p):
        @pl.loop(0, NZ - 1)
        def _(i):
            k = i // 2 + 1
            j = rem(z + jnp.where(rem(i, 2) == 0, k, NZ - k), NZ)
            arrived(owned(p + OWN, j), agz.at[p, j])
            spread_owned(p + OWN, j)

    def forwards(p):
        @pl.loop(0, PART)
        def _(k):
            turn = jnp.where(k == 2, 3, jnp.where(k == 3, 2, k))
            forward(p, rem(z // PAIR + turn, PART), k == 0)

    def each(part, *args):
        @pl.loop(0, PART)
        def _(m):
            part(*args, m)

    def step(n, carry):
        first, second = n * OWN, n * OWN + 1
        backward(first)
        forwards(second)
        backward(second)
        each(plane_sum, first)
        each(plane_sum, second)
        step_on(first)
        step_on(second)
        pass_on(first)
        pass_on(second)
        forwards(first + OWN)
        return carry

    lax.fori_loop(0, STEPS - 1, step, 0)

    row = lax.broadcasted_iota(jnp.int32, (8, 128), 0)
    lane = lax.broadcasted_iota(jnp.int32, (8, 128), 1)
    own_lane = y * BLOCK + slot

    last = PHASES - 1
    backward(last - 1)
    forwards(last)
    backward(last)

    inputs[2].wait()
    v = esum[...] / STEPS
    for i in range(OWN):
        v = v - jnp.where((row == i) & (lane == own_lane), slw_ref[i], 0.0)
    e1[...] = v
    for rel in range(1, PEERS + 1):
        push(e1, ex.at[rel - 1], snd.at[5], one.at[3], xypeer(rel))

    each(plane_sum, last - 1)
    arrived(ex, one.at[3])
    total = e1[...]
    for k in range(PEERS):
        total = total + ex[k]
    e2[...] = total
    for dz in range(1, NZ):
        push(e2, ez.at[dz - 1], snd.at[6], one.at[4], zpeer(dz))

    each(plane_sum, last)
    update(last - 1, STEPS - 1, 0)
    update(last, STEPS - 1, 1)
    for i in range(OWN):
        for tt in range(TILES):
            tile = state[i, :, tt * 128 : (tt + 1) * 128]
            fsend[pl.ds(i * TILES + tt, NZ, stride=8), :] = tile[0:NZ]
            fsend[pl.ds(NZ * 8 + i * TILES + tt, NZ, stride=8), :] = tile[NZ:]
    for k in FAR_ZX:
        to = zxpeer(k)
        push(fsend.at[at((to[2] * NZ + to[0]) * 8, 8), :], fall.at[slot], snd.at[8], one.at[2], to)
    fall[slot] = fsend[at(slot * 8, 8), :]

    arrived(ez, one.at[4])
    total = e2[...]
    for k in range(NZ - 1):
        total = total + ez[k]
    e3[...] = -total
    for k in range(1, 4):
        push(e3, el.at[k - 1], snd.at[7], one.at[5], gpeer(k))
    for i in range(OWN):
        lw_ref[i] = jnp.sum(jnp.where((row == i) & (lane == own_lane), -total, 0.0))
    arrived(el, one.at[5])
    used = (row < OWN) & (lane < ROWS)
    lws = [jnp.where(used, v, -jnp.inf) for v in [-total] + [el[k] for k in range(3)]]
    top = jnp.max(jnp.maximum(jnp.maximum(lws[0], lws[1]), jnp.maximum(lws[2], lws[3])))
    mass = jnp.sum(sum(jnp.exp(v - top) for v in lws))
    lr_ref[0] = jnp.max(top + jnp.log(jnp.full((8, 128), mass, F32)) - math.log(4 * OWN * ROWS))

    arrived(fall.at[pl.ds(0, SRC - 1)], one.at[2])
    for src in range(SRC):
        for i in range(OWN):
            for tt in range(TILES):
                c = (src * TILES + tt) * 128
                out_ref[i : i + 1, c : c + 128] = fall[src, i * TILES + tt : i * TILES + tt + 1, :]

    left(iall.at[:, pl.ds(0, SRC - 1)], snd.at[0])
    left(dpack.at[pl.ds(0, SRC - 1)], snd.at[1])
    left(s_all.at[:, :, :, pl.ds(0, SENT)], snd.at[2])
    left(zx, snd.at[3])
    left(zx.at[pl.ds(0, PHASES - OWN)], snd.at[4])
    left(ex, snd.at[5])
    left(ez, snd.at[6])
    left(el, snd.at[7])
    left(fall.at[pl.ds(0, SRC - 1)], snd.at[8])
    for p in range(PHASES):
        left(g_all.at[p, :, :, pl.ds(0, SENT)], sndg.at[p])


def per_device(start_state, start_log_weight, noise, first_weight, second_weight, third_weight):
    smem = pl.BlockSpec(memory_space=pltpu.SMEM)
    hbm = pl.BlockSpec(memory_space=pl.ANY)
    tile = (8, 128)
    state, log_weight, log_ratio = pl.pallas_call(
        kernel,
        out_shape=(
            jax.ShapeDtypeStruct((OWN, D), F32),
            jax.ShapeDtypeStruct((OWN,), F32),
            jax.ShapeDtypeStruct((1,), F32),
        ),
        in_specs=[hbm] * 6,
        out_specs=(pl.BlockSpec(memory_space=pltpu.VMEM), smem, smem),
        scratch_shapes=[
            pltpu.VMEM((OWN, D), F32),
            pltpu.SMEM((OWN,), F32),
            pltpu.VMEM((STEPS, OWN, D), BF16),
            pltpu.VMEM((PART, 3, PAD, CHUNK), BF16),
            pltpu.VMEM((PHASES, PART, ROWS, CHUNK), BF16),
            pltpu.VMEM((PHASES, PART, ROWS, CHUNK), BF16),
            pltpu.VMEM((PHASES, PART, PEERS, BLOCK, SIDE), BF16),
            pltpu.VMEM((PHASES, PART, BLOCK, SIDE), BF16),
            pltpu.VMEM((PHASES, NZ - 1, BLOCK, COLS), BF16),
            pltpu.VMEM((OWN, BLOCK, COLS), F32),
            pltpu.VMEM((OWN, BLOCK, COLS), F32),
            pltpu.VMEM((3 * PAD, ROWS), F32),
            pltpu.VMEM((3 * PAD, ROWS), BF16),
            pltpu.VMEM(tile, F32),
            pltpu.VMEM((NX, OWN, 16, 128), F32),
            pltpu.VMEM((OWN, SRC, 16, 128), BF16),
            pltpu.VMEM((OWN, NX, 16, 128), BF16),
            pltpu.VMEM((SRC * 16, 128), F32),
            pltpu.VMEM((SRC, 16, 128), F32),
            pltpu.VMEM((SRC * 16, 128), F32),
            pltpu.VMEM((SRC * 8, 128), F32),
            pltpu.VMEM((SRC, 8, 128), F32),
            pltpu.VMEM(tile, F32),
            pltpu.VMEM((PEERS, *tile), F32),
            pltpu.VMEM(tile, F32),
            pltpu.VMEM((NZ - 1, *tile), F32),
            pltpu.VMEM(tile, F32),
            pltpu.VMEM((3, *tile), F32),
            pltpu.SemaphoreType.DMA((3,)),
            pltpu.SemaphoreType.DMA((PART, 3, NX)),
            pltpu.SemaphoreType.DMA((PHASES, PART)),
            pltpu.SemaphoreType.DMA((PHASES - OWN, NZ)),
            pltpu.SemaphoreType.DMA((PHASES, PART)),
            pltpu.SemaphoreType.DMA((PHASES,)),
            pltpu.SemaphoreType.DMA((8,)),
            pltpu.SemaphoreType.DMA((9,)),
            pltpu.SemaphoreType.DMA((PHASES,)),
        ],
        compiler_params=pltpu.CompilerParams(
            collective_id=0, has_side_effects=True, vmem_limit_bytes=67043328
        ),
    )(start_state, start_log_weight, noise, first_weight, second_weight, third_weight)
    return state, log_weight, log_ratio[0]


def solution(mesh):
    torus = Mesh(mesh.devices.reshape(8, 4, 2, 2, 2), AXES)
    placed = (
        P(BLK_GRP, None),
        P(BLK_GRP),
        P(None, BLK_GRP, None),
        P(BLK, None),
        P(BLK, None),
        P(BLK, None),
    )
    return jax.shard_map(
        per_device,
        mesh=torus,
        in_specs=placed,
        out_specs=(P(BLK_GRP, None), P(BLK_GRP), P()),
        check_vma=False,
    )
```

```python
import math

import jax
import jax.numpy as jnp
from jax import lax
from jax.experimental import pallas as pl
from jax.experimental.pallas import tpu as pltpu
from jax.sharding import Mesh
from jax.sharding import PartitionSpec as P

BLK = ("blk_0", "blk_1", "blk_2")
BLK_GRP = ("blk_0", "blk_1", "blk_2", "grp_0", "grp_1")
AXES = BLK_GRP
MESH = pl.DeviceIdType.MESH
F32 = jnp.float32
BF16 = jnp.bfloat16

NZ, NY, NX = 8, 4, 2
OWN = 2
BLOCK = NX * NZ
ROWS = NY * BLOCK
STEPS = 3
PHASES = STEPS * OWN
D = 4096
COLS = D // (NX * NZ)
PART = 4
SIDE = D // (NX * PART)
CHUNK = NX * SIDE
PAIR = SIDE // COLS
TILES = COLS // 128
SRC = NX * NZ
PAD = 256
PEERS = NY * NX - 1
SENT = CHUNK * PEERS // (PEERS + 1)
FAR_XY = (5, 4, 3, 7, 2, 6, 1)
FAR_Z = (4, 3, 5, 2, 6, 1, 7)
FAR_ZX = tuple(NX * dz + 1 for dz in FAR_Z[:3]) + tuple(NX * dz for dz in FAR_Z[:3]) + tuple(
    NX * dz + dx for dz in FAR_Z[3:] for dx in (1, 0)
) + (1,)


def rem(a, n):
    return lax.rem(a, n)


def at(start, size):
    return pl.ds(pl.multiple_of(start, size), size)


def kernel(
    start_hbm, slw_hbm, noise_hbm, w1_ref, w2_ref, w3_ref,
    out_ref, lw_ref, lr_ref,
    start_ref, slw_ref, noise_ref,
    w, s_all, g_all, rx, zs, zx, zown, state, acc, fac, esum,
    ipack, iall, conv, wide, dpack, dall, fsend, fall, e1, ex, e2, ez, e3, el,
    insem, wsem, agx, agz, rxs, zxs, one, snd, sndg,
):
    z, y, xh, xl, core = (lax.axis_index(name) for name in AXES)
    width = w1_ref.shape[0]
    rows_y = at(y * BLOCK, BLOCK)
    side = at(xh * SIDE, SIDE)
    slot = xh * NZ + z

    def zpeer(dz):
        return (rem(z + dz, NZ), y, xh, xl, core)

    def xypeer(rel):
        dy, dx = divmod(rel, NX)
        return (z, rem(y + dy, NY), rem(xh + dx, NX), rem(xl + dx, NX), core)

    def zxpeer(k):
        dz, dx = divmod(k, NX)
        return (rem(z + dz, NZ), y, rem(xh + dx, NX), rem(xl + dx, NX), core)

    def gpeer(k):
        dl, dc = divmod(k, 2)
        return (z, y, xh, rem(xl + dl, 2), rem(core + dc, 2))

    def push(src, dst, send, recv, to):
        pltpu.make_async_remote_copy(
            src_ref=src, dst_ref=dst, send_sem=send, recv_sem=recv, device_id=to, device_id_type=MESH
        ).start()

    def arrived(ref, recv):
        pltpu.make_async_remote_copy(
            src_ref=ref, dst_ref=ref, send_sem=snd.at[0], recv_sem=recv,
            device_id=zpeer(1), device_id_type=MESH,
        ).wait_recv()

    def left(ref, send):
        pltpu.make_async_remote_copy(
            src_ref=ref, dst_ref=ref, send_sem=send, recv_sem=one.at[0],
            device_id=zpeer(1), device_id_type=MESH,
        ).wait_send()

    inputs = (
        pltpu.make_async_copy(start_hbm, start_ref, insem.at[0]),
        pltpu.make_async_copy(noise_hbm, noise_ref, insem.at[1]),
        pltpu.make_async_copy(slw_hbm, slw_ref, insem.at[2]),
    )
    for copy in inputs:
        copy.start()

    barrier = pltpu.get_barrier_semaphore()
    greeted = (
        [zxpeer(k) for k in range(1, SRC)]
        + [xypeer(r) for r in range(2, PEERS + 1)]
        + [gpeer(k) for k in range(1, 4)]
    )
    for to in greeted:
        pl.semaphore_signal(barrier, inc=1, device_id=to, device_id_type=MESH)

    weights = (w1_ref, w2_ref, w3_ref)

    def weight_copy(m, k, half):
        return pltpu.make_async_copy(
            weights[k].at[:, at(half * (D // NX) + m * SIDE, SIDE)],
            w.at[m, k, pl.ds(0, width), pl.ds(half * SIDE, SIDE)],
            wsem.at[m, k, half],
        )

    @pl.loop(0, PART)
    def _(m):
        for k in range(3):
            for half in range(NX):
                weight_copy(m, k, half).start()

    per_side = D // NX // 128
    inputs[0].wait()
    for t in range(D // 128):
        v = start_ref[:, t * 128 : (t + 1) * 128]
        xs, tl = divmod(t, per_side)
        for i in range(OWN):
            ipack[xs, i, tl : tl + 1, :] = v[i : i + 1]
            r = i * TILES + tl % TILES
            dpack[xs * NZ + tl // TILES, r : r + 1, :] = v[i : i + 1]
    for i in range(OWN):
        conv[i] = ipack[:, i].astype(BF16)
        iall[i, slot] = conv[i, xh]

    pl.semaphore_wait(barrier, len(greeted))

    for i in range(OWN):
        for k in FAR_ZX:
            to = zxpeer(k)
            push(conv.at[i, to[2]], iall.at[i, slot], snd.at[0], one.at[6 + i], to)

    inputs[1].wait()
    for k in range(STEPS):
        for t in range(D // 128):
            v = noise_ref[k, :, t * 128 : (t + 1) * 128].astype(F32)
            xs, tl = divmod(t, per_side)
            for i in range(OWN):
                r = (k + 1) * OWN * TILES + i * TILES + tl % TILES
                dpack[xs * NZ + tl // TILES, r : r + 1, :] = v[i : i + 1]
    dall[at(slot * 16, 16), :] = dpack[slot]
    for k in FAR_ZX:
        to = zxpeer(k)
        push(dpack.at[to[2] * NZ + to[0]], dall.at[at(slot * 16, 16), :], snd.at[1], one.at[1], to)

    @pl.loop(0, PART)
    def _(m):
        for k in range(3):
            w[m, k, width:PAD, :] = jnp.zeros((PAD - width, CHUNK), BF16)

    esum[...] = jnp.zeros_like(esum)
    fsend[...] = jnp.zeros_like(fsend)

    def spread(p, m):
        for rel in FAR_XY:
            block = s_all.at[p, m, rows_y, side]
            push(block, block, snd.at[2], agx.at[p, m], xypeer(rel))

    def forward(p, m, start):
        arrived(s_all.at[p, m, :, pl.ds(0, SENT)], agx.at[p, m])
        term = lax.dot_general(
            w[m].reshape(3 * PAD, CHUNK), s_all[p, m], (((1,), (1,)), ((), ())), preferred_element_type=F32
        )

        @pl.when(start)
        def _():
            acc[...] = term

        @pl.when(jnp.logical_not(start))
        def _():
            acc[...] += term

    def gathered(ref, row, stride):
        lo = ref[pl.ds(row, NZ, stride=stride), :]
        hi = ref[pl.ds(NZ * stride + row, NZ, stride=stride), :]
        return jnp.concatenate([lo, hi], axis=0)

    for i in range(OWN):
        arrived(iall.at[i, pl.ds(0, SRC - 1)], one.at[6 + i])
        wide[...] = iall[i].reshape(SRC * per_side, 128).astype(F32)
        for tl in range(per_side):
            m, pos = divmod(tl, SIDE // 128)
            lanes = at(xh * SIDE + pos * 128, 128)
            s_all[i, m, rows_y, lanes] = gathered(wide, tl, per_side).astype(BF16)
            if pos == SIDE // 128 - 1:
                spread(i, m)

    arrived(dall.at[pl.ds(0, 16 * (SRC - 1)), :], one.at[1])
    for i in range(OWN):
        for tt in range(TILES):
            state[i, :, tt * 128 : (tt + 1) * 128] = gathered(dall, i * TILES + tt, 16)

    @pl.loop(0, PART)
    def _(m):
        for k in range(3):
            for half in range(NX):
                weight_copy(m, k, half).wait()
        forward(0, m, m == 0)

    def factors(p):
        h = rem(p, OWN)

        def part(q, total):
            r = q * 64
            pa, pb, pc = (acc[at(k * PAD + r, 64), :] for k in range(3))
            e = jnp.exp(-jnp.abs(pa))
            soft = jnp.maximum(pa, 0.0) + jnp.log1p(e)
            inv = 1.0 / (1.0 + e)
            sig = jnp.where(pa >= 0, inv, e * inv)
            tan = jnp.tanh(pb)
            st = soft * tan
            fac[at(r, 64), :] = (sig * tan * pc).astype(BF16)
            fac[at(PAD + r, 64), :] = (soft * (1.0 - tan * tan) * pc).astype(BF16)
            fac[at(2 * PAD + r, 64), :] = st.astype(BF16)
            return total + jnp.sum(st * pc, axis=0, keepdims=True)

        total = lax.fori_loop(0, PAD // 64, part, jnp.zeros((1, ROWS), F32))
        esum[pl.ds(h, 1), 0:ROWS] += total

    def backward(p):
        factors(p)

        @pl.loop(0, PART)
        def _(m):
            g = lax.dot_general(
                fac[...], w[m].reshape(3 * PAD, CHUNK), (((0,), (0,)), ((), ())), preferred_element_type=F32
            )
            g_all[p, m] = g.astype(BF16)
            for rel in FAR_XY:
                to = xypeer(rel)
                block = g_all.at[p, m, at(to[1] * BLOCK, BLOCK), at(to[2] * SIDE, SIDE)]
                push(block, rx.at[p, m, rel - 1], sndg.at[p], rxs.at[p, m], to)

    def plane_sum(p, m):
        arrived(rx.at[p, m], rxs.at[p, m])
        total = g_all[p, m, rows_y, side].astype(F32)
        for k in range(PEERS):
            total = total + rx[p, m, k].astype(F32)
        zs[p, m] = total.astype(BF16)
        for jj in range(PAIR):
            j = m * PAIR + jj

            @pl.when(j == z)
            def _():
                zown[rem(p, OWN)] = total[:, jj * COLS : (jj + 1) * COLS]

            @pl.when(j != z)
            def _():
                dz = rem(j - z + NZ, NZ)
                push(
                    zs.at[p, m, :, pl.ds(jj * COLS, COLS)], zx.at[p, dz - 1], snd.at[3], zxs.at[p],
                    (j, y, xh, xl, core),
                )

    def update(p, n, h):
        arrived(zx.at[p], zxs.at[p])
        grad = zown[h]
        for k in range(NZ - 1):
            grad = grad + zx[p, k].astype(F32)
        beta = jnp.asarray(n + 1, jnp.int32).astype(F32) / STEPS
        for tt in range(TILES):
            cols = slice(tt * 128, (tt + 1) * 128)
            extra = gathered(dall, ((n + 1) * OWN + h) * TILES + tt, 16)
            old = state[h, :, cols]
            state[h, :, cols] = old - 0.05 * (old + beta * grad[:, cols]) + math.sqrt(0.1) * extra

    def owned(p, j):
        return s_all.at[p, j // PAIR, rows_y, at(xh * SIDE + rem(j, PAIR) * COLS, COLS)]

    def spread_owned(p, j):
        for rel in FAR_XY:
            push(owned(p, j), owned(p, j), snd.at[2], agx.at[p, j // PAIR], xypeer(rel))

    def step_on(p):
        n, h = p // OWN, rem(p, OWN)
        update(p, n, h)

        block = owned(p + OWN, z)
        block[...] = state[h].astype(BF16)
        for dz in FAR_Z:
            push(block, block, snd.at[4], agz.at[p, z], zpeer(dz))
        spread_owned(p + OWN, z)

    def pass_on(p):
        @pl.loop(0, NZ - 1)
        def _(i):
            k = i // 2 + 1
            j = rem(z + jnp.where(rem(i, 2) == 0, k, NZ - k), NZ)
            arrived(owned(p + OWN, j), agz.at[p, j])
            spread_owned(p + OWN, j)

    def forwards(p):
        @pl.loop(0, PART)
        def _(k):
            turn = jnp.where(k == 2, 3, jnp.where(k == 3, 2, k))
            forward(p, rem(z // PAIR + turn, PART), k == 0)

    def each(part, *args):
        @pl.loop(0, PART)
        def _(m):
            part(*args, m)

    def step(n, carry):
        first, second = n * OWN, n * OWN + 1
        backward(first)
        forwards(second)
        backward(second)
        each(plane_sum, first)
        @pl.loop(0, PART - 1)
        def _(m):
            plane_sum(second, m)

        step_on(first)
        plane_sum(second, PART - 1)
        step_on(second)
        pass_on(first)
        pass_on(second)
        forwards(first + OWN)
        return carry

    lax.fori_loop(0, STEPS - 1, step, 0)

    row = lax.broadcasted_iota(jnp.int32, (8, 128), 0)
    lane = lax.broadcasted_iota(jnp.int32, (8, 128), 1)
    own_lane = y * BLOCK + slot

    last = PHASES - 1
    backward(last - 1)
    forwards(last)
    backward(last)

    inputs[2].wait()
    v = esum[...] / STEPS
    for i in range(OWN):
        v = v - jnp.where((row == i) & (lane == own_lane), slw_ref[i], 0.0)
    e1[...] = v
    for rel in range(1, PEERS + 1):
        push(e1, ex.at[rel - 1], snd.at[5], one.at[3], xypeer(rel))

    each(plane_sum, last - 1)
    arrived(ex, one.at[3])
    total = e1[...]
    for k in range(PEERS):
        total = total + ex[k]
    e2[...] = total
    for dz in range(1, NZ):
        push(e2, ez.at[dz - 1], snd.at[6], one.at[4], zpeer(dz))

    each(plane_sum, last)
    update(last - 1, STEPS - 1, 0)
    update(last, STEPS - 1, 1)
    for i in range(OWN):
        for tt in range(TILES):
            tile = state[i, :, tt * 128 : (tt + 1) * 128]
            fsend[pl.ds(i * TILES + tt, NZ, stride=8), :] = tile[0:NZ]
            fsend[pl.ds(NZ * 8 + i * TILES + tt, NZ, stride=8), :] = tile[NZ:]
    for k in FAR_ZX:
        to = zxpeer(k)
        push(fsend.at[at((to[2] * NZ + to[0]) * 8, 8), :], fall.at[slot], snd.at[8], one.at[2], to)
    fall[slot] = fsend[at(slot * 8, 8), :]

    arrived(ez, one.at[4])
    total = e2[...]
    for k in range(NZ - 1):
        total = total + ez[k]
    e3[...] = -total
    for k in range(1, 4):
        push(e3, el.at[k - 1], snd.at[7], one.at[5], gpeer(k))
    for i in range(OWN):
        lw_ref[i] = jnp.sum(jnp.where((row == i) & (lane == own_lane), -total, 0.0))
    arrived(el, one.at[5])
    used = (row < OWN) & (lane < ROWS)
    lws = [jnp.where(used, v, -jnp.inf) for v in [-total] + [el[k] for k in range(3)]]
    top = jnp.max(jnp.maximum(jnp.maximum(lws[0], lws[1]), jnp.maximum(lws[2], lws[3])))
    mass = jnp.sum(sum(jnp.exp(v - top) for v in lws))
    lr_ref[0] = jnp.max(top + jnp.log(jnp.full((8, 128), mass, F32)) - math.log(4 * OWN * ROWS))

    arrived(fall.at[pl.ds(0, SRC - 1)], one.at[2])
    for src in range(SRC):
        for i in range(OWN):
            for tt in range(TILES):
                c = (src * TILES + tt) * 128
                out_ref[i : i + 1, c : c + 128] = fall[src, i * TILES + tt : i * TILES + tt + 1, :]

    left(iall.at[:, pl.ds(0, SRC - 1)], snd.at[0])
    left(dpack.at[pl.ds(0, SRC - 1)], snd.at[1])
    left(s_all.at[:, :, :, pl.ds(0, SENT)], snd.at[2])
    left(zx, snd.at[3])
    left(zx.at[pl.ds(0, PHASES - OWN)], snd.at[4])
    left(ex, snd.at[5])
    left(ez, snd.at[6])
    left(el, snd.at[7])
    left(fall.at[pl.ds(0, SRC - 1)], snd.at[8])
    for p in range(PHASES):
        left(g_all.at[p, :, :, pl.ds(0, SENT)], sndg.at[p])


def per_device(start_state, start_log_weight, noise, first_weight, second_weight, third_weight):
    smem = pl.BlockSpec(memory_space=pltpu.SMEM)
    hbm = pl.BlockSpec(memory_space=pl.ANY)
    tile = (8, 128)
    state, log_weight, log_ratio = pl.pallas_call(
        kernel,
        out_shape=(
            jax.ShapeDtypeStruct((OWN, D), F32),
            jax.ShapeDtypeStruct((OWN,), F32),
            jax.ShapeDtypeStruct((1,), F32),
        ),
        in_specs=[hbm] * 6,
        out_specs=(pl.BlockSpec(memory_space=pltpu.VMEM), smem, smem),
        scratch_shapes=[
            pltpu.VMEM((OWN, D), F32),
            pltpu.SMEM((OWN,), F32),
            pltpu.VMEM((STEPS, OWN, D), BF16),
            pltpu.VMEM((PART, 3, PAD, CHUNK), BF16),
            pltpu.VMEM((PHASES, PART, ROWS, CHUNK), BF16),
            pltpu.VMEM((PHASES, PART, ROWS, CHUNK), BF16),
            pltpu.VMEM((PHASES, PART, PEERS, BLOCK, SIDE), BF16),
            pltpu.VMEM((PHASES, PART, BLOCK, SIDE), BF16),
            pltpu.VMEM((PHASES, NZ - 1, BLOCK, COLS), BF16),
            pltpu.VMEM((OWN, BLOCK, COLS), F32),
            pltpu.VMEM((OWN, BLOCK, COLS), F32),
            pltpu.VMEM((3 * PAD, ROWS), F32),
            pltpu.VMEM((3 * PAD, ROWS), BF16),
            pltpu.VMEM(tile, F32),
            pltpu.VMEM((NX, OWN, 16, 128), F32),
            pltpu.VMEM((OWN, SRC, 16, 128), BF16),
            pltpu.VMEM((OWN, NX, 16, 128), BF16),
            pltpu.VMEM((SRC * 16, 128), F32),
            pltpu.VMEM((SRC, 16, 128), F32),
            pltpu.VMEM((SRC * 16, 128), F32),
            pltpu.VMEM((SRC * 8, 128), F32),
            pltpu.VMEM((SRC, 8, 128), F32),
            pltpu.VMEM(tile, F32),
            pltpu.VMEM((PEERS, *tile), F32),
            pltpu.VMEM(tile, F32),
            pltpu.VMEM((NZ - 1, *tile), F32),
            pltpu.VMEM(tile, F32),
            pltpu.VMEM((3, *tile), F32),
            pltpu.SemaphoreType.DMA((3,)),
            pltpu.SemaphoreType.DMA((PART, 3, NX)),
            pltpu.SemaphoreType.DMA((PHASES, PART)),
            pltpu.SemaphoreType.DMA((PHASES - OWN, NZ)),
            pltpu.SemaphoreType.DMA((PHASES, PART)),
            pltpu.SemaphoreType.DMA((PHASES,)),
            pltpu.SemaphoreType.DMA((8,)),
            pltpu.SemaphoreType.DMA((9,)),
            pltpu.SemaphoreType.DMA((PHASES,)),
        ],
        compiler_params=pltpu.CompilerParams(
            collective_id=0, has_side_effects=True, vmem_limit_bytes=67043328
        ),
    )(start_state, start_log_weight, noise, first_weight, second_weight, third_weight)
    return state, log_weight, log_ratio[0]


def solution(mesh):
    torus = Mesh(mesh.devices.reshape(8, 4, 2, 2, 2), AXES)
    placed = (
        P(BLK_GRP, None),
        P(BLK_GRP),
        P(None, BLK_GRP, None),
        P(BLK, None),
        P(BLK, None),
        P(BLK, None),
    )
    return jax.shard_map(
        per_device,
        mesh=torus,
        in_specs=placed,
        out_specs=(P(BLK_GRP, None), P(BLK_GRP), P()),
        check_vma=False,
    )
```
